128 devices in a mesh: ep: 8 (over y, core), fs: 16 (over z, x).
Axes of the slice: x: 4, y: 4, z: 4, core: 2. Of those that a mesh axis runs over, the one named last changes fastest.
Arguments:
- grads: bfloat16 [8, 8, 256, 14336], P('ep', None, 'fs'), may hold values from -64 to 64
- counts: int32 [8, 8], replicated, may hold values from 16 to 2047
- weight: bfloat16 [8, 256, 14336], P('ep', 'fs'), may hold values from -3 to 3
- mom: float32 [8, 256, 14336], P('ep', 'fs'), may hold values from -64 to 64
- second: float32 [8, 256, 14336], P('ep', 'fs'), may hold values from 0.1 to 10
- in_weight: float32 [6, 32], replicated, may hold values from -2.5 to 2.5
- in_bias: float32 [32], replicated, may hold values from -3 to 3
- out_weight: float32 [32, 2], replicated, may hold values from -1 to 1
- out_bias: float32 [2], replicated, may hold values from -3 to 3
Outputs:
- new_weight: bfloat16 [8, 256, 14336], P('ep')
- new_mom: float32 [8, 256, 14336], P('ep', 'fs')
- new_second: float32 [8, 256, 14336], P('ep', 'fs')
The draws below stay inside these ranges and needn't reach their ends.
All inputs are finite; a program needn't handle non-finite values.
Results may differ from the reference program's by a relative error of at most 0.0019.
Values may be sent and summed in bfloat16 or wider, within the bound.
A program may use at most 64 MiB of HBM per device.

```python
import math
import jax
import jax.numpy as jnp
from jax import lax

FF = 14336
EXPERTS = 8
R = 256
HID = 32
FEATS = 6


def scaled_field(key, field_shape, magnitude):
    key_noise, key_cols = jax.random.split(key, 2)
    row_scale = 10.0 ** (jnp.arange(R, dtype=jnp.float32) / R)
    col_scale = jnp.exp(jax.random.uniform(key_cols, (FF,), jnp.float32, 0.0, math.log(10.0)))
    noise_field = jnp.clip(jax.random.normal(key_noise, field_shape, jnp.float32), -6.0, 6.0)
    return magnitude * noise_field * row_scale[:, None] * col_scale


def draw_grads(key, part):
    return scaled_field(jax.random.fold_in(key, 101), (EXPERTS, EXPERTS, R, FF), 0.01).astype(jnp.bfloat16)


def draw_mom(key, part):
    return scaled_field(jax.random.fold_in(key, 202), (EXPERTS, R, FF), 0.01)


def touch_ends(array, stream_key, least, top_value):
    index_at = [jax.random.randint(jax.random.fold_in(stream_key, axis), (), 0, length) for axis, length in enumerate(array.shape)]
    longest = array.shape.index(max(array.shape))
    neighbour = index_at[:longest] + [(index_at[longest] + 1) % array.shape[longest]] + index_at[longest + 1:]
    return array.at[tuple(index_at)].set(least).at[tuple(neighbour)].set(top_value)


def level_of(rng, shape, cuts, smallest, top_value):
    factor_of = 1.0
    for position, shards_of in cuts:
        draws = jax.random.uniform(jax.random.fold_in(jax.random.fold_in(rng, 6), position), (shards_of,), jnp.float32, smallest / len(cuts), top_value / len(cuts))
        factor_of = factor_of * jnp.repeat(jnp.exp(draws), shape[position] // shards_of).reshape((-1,) + (1,) * (len(shape) - 1 - position))
    return factor_of


def noise(stream_key, shape, spread, most, cuts=(), held_as=jnp.bfloat16):
    values = jax.random.normal(stream_key, shape, jnp.float32) * spread
    if len(cuts) > 0:
        values = level_of(stream_key, shape, cuts, -0.22, 0.18) * values
    return jnp.clip(values, min=-most, max=most).astype(held_as)


def setup_inputs(seed: int = 0) -> dict:
    key_list = jax.random.split(jax.random.key(seed), 10)
    return {
        "grads": draw_grads(jax.random.fold_in(key_list[9], 71), 0),
        "counts": touch_ends(jax.random.randint(key_list[1], (EXPERTS, EXPERTS), 16, 2048), jax.random.fold_in(key_list[1], 1), 16, 2047).astype(jnp.int32),
        "weight": noise(key_list[2], (EXPERTS, R, FF), 0.5, 3.0, ((0, 8), (1, 16))),
        "mom": draw_mom(jax.random.fold_in(key_list[9], 71), 0),
        "second": jnp.clip(jnp.exp(math.log(10.0) - 4.6051702 * jax.random.uniform(key_list[4], (EXPERTS, R, FF), jnp.float32) ** level_of(key_list[4], (EXPERTS, R, FF), ((0, 8), (1, 16)), -0.2, 0.2)), 0.1, 10.0),
        "in_weight": noise(key_list[5], (FEATS, HID), FEATS ** -0.5, 2.5, (), jnp.float32),
        "in_bias": noise(key_list[6], (HID,), 0.5, 3.0, (), jnp.float32),
        "out_weight": noise(key_list[7], (HID, 2), HID ** -0.5, 1.0, (), jnp.float32),
        "out_bias": noise(key_list[8], (2,), 0.5, 3.0, (), jnp.float32),
    }


MOMENTUM_DECAY = 0.9
SECOND_DECAY = 0.99
NORM_EPS = 1e-06
ROOT_EPS = 1e-08
STEP_SCALE = 0.2
EXP_SCALE = 0.5

def learned_step(gradient, mom_next, second_next, weight, grad_norm, mom_norm, in_weight, in_bias, out_weight, out_bias):
    inv_root = lax.rsqrt(second_next + ROOT_EPS)
    features = jnp.stack([gradient / grad_norm, mom_next / mom_norm, mom_next * inv_root, gradient * inv_root, weight.astype(jnp.float32), jnp.broadcast_to(jnp.log(mom_norm), gradient.shape)])
    hidden = jax.nn.relu(jnp.einsum('fh,fab->hab', in_weight, features, precision=lax.Precision.HIGHEST) + in_bias[:, None, None])
    outputs = jnp.einsum('hk,hab->kab', out_weight, hidden, precision=lax.Precision.HIGHEST) + out_bias[:, None, None]
    update = STEP_SCALE * outputs[0] * jnp.exp(EXP_SCALE * outputs[1])
    return (weight.astype(jnp.float32) - update).astype(jnp.bfloat16)

def reference(grads, counts, weight, mom, second, in_weight, in_bias, out_weight, out_bias):
    counts_f = counts.astype(jnp.float32)
    totals = lax.optimization_barrier(jnp.sum(counts_f, axis=0))
    shares = counts_f / totals[None, :]

    def per_expert(items):
        expert_grads, expert_shares, expert_weight, expert_mom, expert_second = items
        weighted = (expert_shares[:, None, None] * expert_grads.astype(jnp.float32)).astype(jnp.bfloat16)
        weighted = lax.optimization_barrier(weighted)
        gradient = lax.optimization_barrier(jnp.sum(weighted.astype(jnp.float32), axis=0))
        mom_next = MOMENTUM_DECAY * expert_mom + (1.0 - MOMENTUM_DECAY) * gradient
        second_next = SECOND_DECAY * expert_second + (1.0 - SECOND_DECAY) * gradient * gradient
        entries = gradient.shape[0] * gradient.shape[1]
        grad_norm = jnp.sqrt(jnp.sum(gradient * gradient) / entries + NORM_EPS)
        mom_norm = jnp.sqrt(jnp.sum(mom_next * mom_next) / entries + NORM_EPS)
        updated = learned_step(gradient, mom_next, second_next, expert_weight, grad_norm, mom_norm, in_weight, in_bias, out_weight, out_bias)
        return (updated, mom_next, second_next)
    new_weight, new_mom, new_second = lax.map(per_expert, (jnp.swapaxes(grads, 0, 1), shares.T, weight, mom, second))
    return (new_weight, new_mom, new_second)
```

```python
import functools

import jax
import jax.numpy as jnp
from jax import lax
from jax.experimental import pallas as pl
from jax.experimental.pallas import tpu as pltpu
from jax.sharding import PartitionSpec as P

MOMENTUM_DECAY = 0.9
SECOND_DECAY = 0.99
NORM_EPS = 1e-06
ROOT_EPS = 1e-08
STEP_SCALE = 0.2
EXP_SCALE = 0.5
LANES = 128
CORES = 2
SIDE = 4
CHUNKS = 16
PIECES = 7
LAG_ONE = 3
LAG_TWO = 6
LAG_THREE = 9
GATE_PIECE = 5
VMEM_BYTES = 67043328 - 9175040


def largest_divisor(number, most):
    return max(d for d in range(1, most + 1) if number % d == 0)


def tile_width(columns, most):
    return LANES * largest_divisor(columns // LANES, most // LANES)


def remote(src, dst, send_sem, recv_sem, axis, peer):
    return pltpu.make_async_remote_copy(
        src_ref=src,
        dst_ref=dst,
        send_sem=send_sem,
        recv_sem=recv_sem,
        device_id={axis: peer},
        device_id_type=pl.DeviceIdType.MESH,
    )


def kernel(
    ring,
    counts_hbm,
    in_weight_hbm,
    in_bias_hbm,
    out_weight_hbm,
    out_bias_hbm,
    grads_hbm,
    weight_hbm,
    mom_hbm,
    second_hbm,
    gathered_out,
    mom_out,
    second_out,
    counts,
    in_weight,
    in_bias,
    out_weight,
    out_bias,
    grads,
    weight,
    pair_out,
    pair_in,
    ring_out,
    ring_in,
    gradient,
    sums,
    bias,
    small_sem,
    slab_sem,
    param_sem,
    pair_send,
    pair_recv,
    ring_send,
    ring_recv,
    gate,
    sum_send,
    sum_recv,
    row_send,
    pass_recv,
    last_recv,
):
    gathered = gathered_out.at[0]
    mom = mom_out.at[0]
    second = second_out.at[0]
    groups = ring * CORES
    shards = SIDE * SIDE
    rows, columns = gradient.shape
    units = in_bias.shape[0]
    me_group = lax.axis_index("ep")
    me = lax.axis_index("fs")
    y = me_group // CORES
    core = me_group % CORES
    partner = y * CORES + 1 - core
    z = me // SIDE
    x = me % SIDE

    def group_of(step, which):
        return (y + step) % ring * CORES + which

    small = [
        pltpu.make_async_copy(src, dst, small_sem.at[i])
        for i, (src, dst) in enumerate(
            (
                (counts_hbm, counts),
                (in_weight_hbm, in_weight),
                (in_bias_hbm, in_bias),
                (out_weight_hbm, out_weight),
                (out_bias_hbm, out_bias),
            )
        )
    ]
    for copy in small:
        copy.start()

    def slab(which, step):
        return pltpu.make_async_copy(
            grads_hbm.at[0, group_of(step, which)],
            grads.at[which, step],
            slab_sem.at[which, step],
        )

    for which in range(CORES):
        for step in range(ring):
            slab(which, step).start()
    params = [
        pltpu.make_async_copy(src.at[0], dst, param_sem.at[i])
        for i, (src, dst) in enumerate(
            ((mom_hbm, mom), (second_hbm, second), (weight_hbm, weight))
        )
    ]
    for copy in params:
        copy.start()

    barrier = pltpu.get_barrier_semaphore()
    for peer in [partner] + [group_of(step, core) for step in range(1, ring)]:
        pl.semaphore_signal(
            barrier, inc=1, device_id={"ep": peer}, device_id_type=pl.DeviceIdType.MESH
        )
    for step in range(1, shards):
        pl.semaphore_signal(
            barrier,
            inc=1,
            device_id={"fs": (me + step) % shards},
            device_id_type=pl.DeviceIdType.MESH,
        )
    for copy in small:
        copy.wait()

    pieces = ring_recv.shape[1]
    piece = columns // pieces
    narrow = tile_width(piece, 512)

    def cols_of(p, i):
        return pl.ds(pl.multiple_of(p * piece + i * narrow, narrow), narrow)

    def piece_of(p):
        return pl.ds(pl.multiple_of(p * piece, piece), piece)

    def share_of(expert):
        total = counts[0, expert]
        for s in range(1, groups):
            total = total + counts[s, expert]
        mine = jnp.full((1, LANES), counts[me_group, expert].astype(jnp.float32))
        return (mine / jnp.full((1, LANES), total.astype(jnp.float32)))[:, :1]

    def weighted(share, which, step, cols):
        value = share * grads[which, step, :, cols].astype(jnp.float32)
        return value.astype(jnp.bfloat16)

    for which in range(CORES):
        for step in range(ring):
            slab(which, step).wait()
    pl.semaphore_wait(barrier, 1 + ring - 1 + shards - 1)

    def pair_copy(p):
        return remote(
            pair_out.at[:, :, piece_of(p)],
            pair_in.at[:, :, piece_of(p)],
            pair_send,
            pair_recv.at[p],
            "ep",
            partner,
        )

    def give():
        shares = [share_of(group_of(step, 1 - core)) for step in range(ring)]

        def body(p, carry):
            def weigh(i, inner):
                cols = cols_of(p, i)
                for step in range(ring):
                    pair_out[step, :, cols] = weighted(shares[step], 1 - core, step, cols)
                return inner

            lax.fori_loop(0, piece // narrow, weigh, 0)
            pair_copy(p).start()
            return carry

        lax.fori_loop(0, pieces, body, 0)

    def ring_copy(step, p):
        return remote(
            ring_out.at[step - 1, :, piece_of(p)],
            ring_in.at[step - 1, :, piece_of(p)],
            ring_send.at[step - 1],
            ring_recv.at[step - 1, p],
            "ep",
            group_of(step, core),
        )

    @pl.when(core == 1)
    def _():
        give()
        pl.semaphore_wait(gate, 1)

    shares = [share_of(group_of(step, core)) for step in range(ring)]
    order = sorted(range(1, ring), key=lambda step: abs(2 * step - ring))

    def send_piece(p, carry):
        pair_copy(p).wait_recv()
        for step in order:

            def add(i, inner, step=step):
                cols = cols_of(p, i)
                total = weighted(shares[step], core, step, cols).astype(jnp.float32)
                total = total + pair_in[step, :, cols].astype(jnp.float32)
                ring_out[step - 1, :, cols] = total.astype(jnp.bfloat16)
                return inner

            lax.fori_loop(0, piece // narrow, add, 0)
            ring_copy(step, p).start()
        return carry

    lax.fori_loop(0, pieces, send_piece, 0)

    @pl.when(core == 0)
    def _():
        give()

    for copy in params:
        copy.wait()

    def moments(p, carry):
        for step in range(1, ring):
            ring_copy(step, p).wait_recv()

        @pl.when(jnp.logical_and(core == 0, p == GATE_PIECE))
        def _():
            pl.semaphore_signal(
                gate,
                inc=1,
                device_id={"ep": partner},
                device_id_type=pl.DeviceIdType.MESH,
            )

        def one(i, inner):
            grad_acc, mom_acc = inner
            cols = cols_of(p, i)
            total = weighted(shares[0], core, 0, cols).astype(jnp.float32)
            total = total + pair_in[0, :, cols].astype(jnp.float32)
            for step in range(1, ring):
                total = total + ring_in[step - 1, :, cols].astype(jnp.float32)
            mom_next = MOMENTUM_DECAY * mom[:, cols] + (1.0 - MOMENTUM_DECAY) * total
            gradient[:, cols] = total
            mom[:, cols] = mom_next
            second[:, cols] = (
                SECOND_DECAY * second[:, cols] + (1.0 - SECOND_DECAY) * total * total
            )
            return grad_acc + total * total, mom_acc + mom_next * mom_next

        return lax.fori_loop(0, piece // narrow, one, carry)

    zero = jnp.zeros((rows, narrow), jnp.float32)
    grad_acc, mom_acc = lax.fori_loop(0, pieces, moments, (zero, zero))

    def to_lanes(acc):
        acc = jnp.sum(acc, axis=0, keepdims=True)
        return sum(acc[:, j : j + LANES] for j in range(0, narrow, LANES))

    sums[me, 0:1, :] = to_lanes(grad_acc)
    sums[me, 1:2, :] = to_lanes(mom_acc)
    sum_sends = []
    for step in range(1, shards):
        copy = remote(
            sums.at[me],
            sums.at[me],
            sum_send.at[step - 1],
            sum_recv.at[me],
            "fs",
            (me + step) % shards,
        )
        copy.start()
        sum_sends.append(copy)
    for step in range(1, shards):
        source = (me + step) % shards
        remote(
            sums.at[source],
            sums.at[source],
            sum_send.at[step - 1],
            sum_recv.at[source],
            "fs",
            source,
        ).wait_recv()

    entries = rows * columns * shards
    totals = sums[0]
    for s in range(1, shards):
        totals = totals + sums[s]
    mean = jnp.broadcast_to(jnp.sum(totals, axis=1, keepdims=True) / entries, (2, LANES)) + NORM_EPS
    inverse = lax.rsqrt(mean)
    inv_grad = inverse[0:1, :1]
    inv_mom = inverse[1:2, :1]
    log_mom = jnp.max(0.5 * jnp.log(mean[1:2, :]))
    for h in range(units):
        bias[h] = in_bias[h] + in_weight[5, h] * log_mom

    chunks = pass_recv.shape[1]
    width = columns // chunks
    tile = tile_width(width, 256)

    def learned_step(cols):
        grad = gradient[:, cols]
        mom_next = mom[:, cols]
        old = weight[:, cols].astype(jnp.float32)
        inv_root = lax.rsqrt(second[:, cols] + ROOT_EPS)
        features = (
            grad * inv_grad,
            mom_next * inv_mom,
            mom_next * inv_root,
            grad * inv_root,
            old,
        )
        direction = jnp.full(grad.shape, out_bias[0])
        magnitude = jnp.full(grad.shape, out_bias[1])
        for h in range(units):
            hidden = features[0] * in_weight[0, h] + bias[h]
            for f in range(1, len(features)):
                hidden = hidden + features[f] * in_weight[f, h]
            hidden = jnp.maximum(hidden, 0.0)
            direction = direction + hidden * out_weight[0, h]
            magnitude = magnitude + hidden * out_weight[1, h]
        update = STEP_SCALE * direction * jnp.exp(EXP_SCALE * magnitude)
        return (old - update).astype(jnp.bfloat16)

    def rows_of(source):
        return pl.ds(pl.multiple_of(source * rows, rows), rows)

    def block(source, k):
        return gathered.at[rows_of(source), pl.ds(pl.multiple_of(k * width, width), width)]

    def route(k):
        swap = k % 2
        turn = 1 - 2 * (k // 2 % 2)

        def at(first, after):
            up = (z + 2 * SIDE + first * swap + after * (1 - swap)) % SIDE
            along = (x + 2 * SIDE + first * (1 - swap) + after * swap) % SIDE
            return up * SIDE + along

        return at, turn

    def send(source, k, role, recv, peer):
        remote(block(source, k), block(source, k), row_send.at[role], recv, "fs", peer).start()

    def spread(source, k, role, at, turn):
        send(source, k, role, pass_recv.at[source, k], at(0, turn))
        send(source, k, role, last_recv.at[source], at(0, -turn))

    def arrive(source, k):
        remote(
            block(source, k), block(source, k), row_send.at[0], pass_recv.at[source, k], "fs", source
        ).wait_recv()

    def own(k):
        at, turn = route(k)
        for way in (1, -1):
            send(me, k, 0, pass_recv.at[me, k], at(way, 0))
        spread(me, k, 0, at, turn)

    def relay_one(k):
        at, turn = route(k)
        source = at(-turn, 0)
        arrive(source, k)
        send(source, k, 1, pass_recv.at[source, k], at(turn, 0))
        spread(source, k, 1, at, turn)
        source = at(turn, 0)
        arrive(source, k)
        spread(source, k, 1, at, turn)
        source = at(0, -turn)
        arrive(source, k)
        send(source, k, 1, last_recv.at[source], at(0, turn))

    def relay_two(k):
        at, turn = route(k)
        source = at(2, 0)
        arrive(source, k)
        spread(source, k, 2, at, turn)
        for way in (1, -1):
            source = at(way, -turn)
            arrive(source, k)
            send(source, k, 2, last_recv.at[source], at(0, turn))

    def relay_three(k):
        at, turn = route(k)
        source = at(2, -turn)
        arrive(source, k)
        send(source, k, 3, last_recv.at[source], at(0, turn))

    def turn_of(t, carry):
        for lag, relay in ((LAG_ONE, relay_one), (LAG_TWO, relay_two), (LAG_THREE, relay_three)):
            k = t - lag

            @pl.when(jnp.logical_and(k >= 0, k < chunks))
            def _(k=k, relay=relay):
                relay(k)

        @pl.when(t < chunks)
        def _():
            def one(i, inner):
                cols = pl.ds(pl.multiple_of(t * width + i * tile, tile), tile)
                gathered[rows_of(me), cols] = learned_step(cols)
                return inner

            lax.fori_loop(0, width // tile, one, 0)
            own(t)

        return carry

    lax.fori_loop(0, chunks + LAG_THREE, turn_of, 0)

    remote(pair_out, pair_in, pair_send, pair_recv.at[0], "ep", partner).wait_send()
    for step in range(1, ring):
        remote(
            ring_out.at[step - 1],
            ring_in.at[step - 1],
            ring_send.at[step - 1],
            ring_recv.at[step - 1, 0],
            "ep",
            group_of(step, core),
        ).wait_send()
    for copy in sum_sends:
        copy.wait_send()
    share = {0: 0, 1: chunks // 4, 2: chunks // 2, 3: chunks // 4}
    for up in range(SIDE):
        for along in range(SIDE):
            number = share[up] + share[along]
            if number == 0:
                continue
            source = (z + up) % SIDE * SIDE + (x + along) % SIDE
            part = gathered.at[rows_of(source), pl.ds(0, number * width)]
            remote(part, part, row_send.at[0], last_recv.at[source], "fs", source).wait_recv()
    for role, number in enumerate((4, 6, 4, 1)):
        part = gathered.at[pl.ds(0, number * rows), :]
        remote(
            part, part, row_send.at[role], last_recv.at[me], "fs", (me + 1) % shards
        ).wait_send()


def per_device(groups, grads, counts, weight, mom, second, in_weight, in_bias, out_weight, out_bias):
    rows, columns = mom.shape[1], mom.shape[2]
    ring = groups // CORES
    shards = SIDE * SIDE
    pieces = PIECES
    chunks = CHUNKS
    hbm = pl.BlockSpec(memory_space=pltpu.HBM)
    vmem = pl.BlockSpec(memory_space=pltpu.VMEM)
    return pl.pallas_call(
        functools.partial(kernel, ring),
        out_shape=(
            pltpu.VMEM((1, rows * shards, columns), jnp.bfloat16),
            pltpu.VMEM(mom.shape, jnp.float32),
            pltpu.VMEM(second.shape, jnp.float32),
        ),
        in_specs=[hbm] * 9,
        out_specs=(vmem, vmem, vmem),
        scratch_shapes=[
            pltpu.SMEM(counts.shape, jnp.int32),
            pltpu.SMEM(in_weight.shape, jnp.float32),
            pltpu.SMEM(in_bias.shape, jnp.float32),
            pltpu.SMEM(out_weight.shape[::-1], jnp.float32),
            pltpu.SMEM(out_bias.shape, jnp.float32),
            pltpu.VMEM((CORES, ring, rows, columns), jnp.bfloat16),
            pltpu.VMEM((rows, columns), jnp.bfloat16),
            pltpu.VMEM((ring, rows, columns), jnp.bfloat16),
            pltpu.VMEM((ring, rows, columns), jnp.bfloat16),
            pltpu.VMEM((ring - 1, rows, columns), jnp.bfloat16),
            pltpu.VMEM((ring - 1, rows, columns), jnp.bfloat16),
            pltpu.VMEM((rows, columns), jnp.float32),
            pltpu.VMEM((shards, 2, LANES), jnp.float32),
            pltpu.SMEM((in_bias.shape[0],), jnp.float32),
            pltpu.SemaphoreType.DMA((5,)),
            pltpu.SemaphoreType.DMA((CORES, ring)),
            pltpu.SemaphoreType.DMA((3,)),
            pltpu.SemaphoreType.DMA,
            pltpu.SemaphoreType.DMA((pieces,)),
            pltpu.SemaphoreType.DMA((ring - 1,)),
            pltpu.SemaphoreType.DMA((ring - 1, pieces)),
            pltpu.SemaphoreType.REGULAR,
            pltpu.SemaphoreType.DMA((shards - 1,)),
            pltpu.SemaphoreType.DMA((shards,)),
            pltpu.SemaphoreType.DMA((4,)),
            pltpu.SemaphoreType.DMA((shards, chunks)),
            pltpu.SemaphoreType.DMA((shards,)),
        ],
        compiler_params=pltpu.CompilerParams(
            collective_id=0, has_side_effects=True, vmem_limit_bytes=VMEM_BYTES
        ),
        name="learned_update",
    )(counts, in_weight, in_bias, out_weight.T, out_bias, grads, weight, mom, second)


def solution(mesh):
    in_specs = (
        P("ep", None, "fs", None),
        P(),
        P("ep", "fs", None),
        P("ep", "fs", None),
        P("ep", "fs", None),
        P(),
        P(),
        P(),
        P(),
    )
    out_specs = (P("ep", None, None), P("ep", "fs", None), P("ep", "fs", None))
    body = functools.partial(per_device, mesh.shape["ep"])
    return jax.shard_map(
        body, mesh=mesh, in_specs=in_specs, out_specs=out_specs, check_vma=False
    )
```

```python
import functools

import jax
import jax.numpy as jnp
from jax import lax
from jax.experimental import pallas as pl
from jax.experimental.pallas import tpu as pltpu
from jax.sharding import PartitionSpec as P

MOMENTUM_DECAY = 0.9
SECOND_DECAY = 0.99
NORM_EPS = 1e-06
ROOT_EPS = 1e-08
STEP_SCALE = 0.2
EXP_SCALE = 0.5
LANES = 128
CORES = 2
SIDE = 4
CHUNKS = 16
PIECES = 7
LAG_ONE = 5
LAG_TWO = 10
LAG_THREE = 15
GATE_PIECE = 5
FIRST = 1
CODES = 32767.0
TINY = 1e-30
TILE = 896
STORES = 4
VMEM_BYTES = 67043328 - 9175040


def largest_divisor(number, most):
    return max(d for d in range(1, most + 1) if number % d == 0)


def tile_width(columns, most):
    return LANES * largest_divisor(columns // LANES, most // LANES)


def remote(src, dst, send_sem, recv_sem, axis, peer):
    return pltpu.make_async_remote_copy(
        src_ref=src,
        dst_ref=dst,
        send_sem=send_sem,
        recv_sem=recv_sem,
        device_id={axis: peer},
        device_id_type=pl.DeviceIdType.MESH,
    )


def kernel(
    ring,
    counts_hbm,
    in_weight_hbm,
    in_bias_hbm,
    out_weight_hbm,
    out_bias_hbm,
    grads_hbm,
    weight_hbm,
    mom_hbm,
    second_hbm,
    gathered_out,
    mom_out,
    second_out,
    counts,
    in_weight,
    in_bias,
    out_weight,
    out_bias,
    grads,
    weight,
    pair_out,
    pair_in,
    ring_out,
    ring_in,
    scale_out,
    scale_in,
    gradient,
    sums,
    layer,
    small_sem,
    slab_sem,
    param_sem,
    pair_send,
    pair_recv,
    ring_send,
    ring_recv,
    scale_send,
    scale_recv,
    gate,
    sum_send,
    sum_recv,
    row_send,
    pass_recv,
    last_recv,
):
    gathered = gathered_out.at[0]
    mom = mom_out.at[0]
    second = second_out.at[0]
    groups = ring * CORES
    shards = SIDE * SIDE
    rows, columns = gradient.shape
    units = in_bias.shape[0]
    me_group = lax.axis_index("ep")
    me = lax.axis_index("fs")
    y = me_group // CORES
    core = me_group % CORES
    partner = y * CORES + 1 - core
    z = me // SIDE
    x = me % SIDE

    def group_of(step, which):
        return (y + step) % ring * CORES + which

    small = [
        pltpu.make_async_copy(src, dst, small_sem.at[i])
        for i, (src, dst) in enumerate(
            (
                (counts_hbm, counts),
                (in_weight_hbm, in_weight),
                (in_bias_hbm, in_bias),
                (out_weight_hbm, out_weight),
                (out_bias_hbm, out_bias),
            )
        )
    ]
    for copy in small:
        copy.start()

    def slab(which, step):
        return pltpu.make_async_copy(
            grads_hbm.at[0, group_of(step, which)],
            grads.at[which, step],
            slab_sem.at[which, step],
        )

    for which in (FIRST, 1 - FIRST):
        for step in range(ring):
            slab(which, step).start()
    params = [
        pltpu.make_async_copy(src.at[0], dst, param_sem.at[i])
        for i, (src, dst) in enumerate(
            ((mom_hbm, mom), (second_hbm, second), (weight_hbm, weight))
        )
    ]
    for copy in params:
        copy.start()

    barrier = pltpu.get_barrier_semaphore()
    for peer in [partner] + [group_of(step, core) for step in range(1, ring)]:
        pl.semaphore_signal(
            barrier, inc=1, device_id={"ep": peer}, device_id_type=pl.DeviceIdType.MESH
        )
    for step in range(1, shards):
        pl.semaphore_signal(
            barrier,
            inc=1,
            device_id={"fs": (me + step) % shards},
            device_id_type=pl.DeviceIdType.MESH,
        )
    for copy in small:
        copy.wait()

    pieces = ring_recv.shape[1]
    piece = columns // pieces
    narrow = tile_width(piece, 512)

    def cols_of(p, i):
        return pl.ds(pl.multiple_of(p * piece + i * narrow, narrow), narrow)

    def piece_of(p):
        return pl.ds(pl.multiple_of(p * piece, piece), piece)

    def share_of(expert):
        total = counts[0, expert]
        for s in range(1, groups):
            total = total + counts[s, expert]
        mine = jnp.full((1, LANES), counts[me_group, expert].astype(jnp.float32))
        return (mine / jnp.full((1, LANES), total.astype(jnp.float32)))[:, :1]

    def weighted(share, which, step, cols):
        value = share * grads[which, step, :, cols].astype(jnp.float32)
        return value.astype(jnp.bfloat16)

    for which in range(CORES):
        for step in range(ring):
            slab(which, step).wait()
    pl.semaphore_wait(barrier, 1 + ring - 1 + shards - 1)

    def pair_copy(p):
        return remote(
            pair_out.at[:, :, piece_of(p)],
            pair_in.at[:, :, piece_of(p)],
            pair_send,
            pair_recv.at[p],
            "ep",
            partner,
        )

    def give():
        shares = [share_of(group_of(step, 1 - core)) for step in range(ring)]

        def body(p, carry):
            def weigh(i, inner):
                cols = cols_of(p, i)
                for step in range(ring):
                    pair_out[step, :, cols] = weighted(shares[step], 1 - core, step, cols)
                return inner

            lax.fori_loop(0, piece // narrow, weigh, 0)
            pair_copy(p).start()
            return carry

        lax.fori_loop(0, pieces, body, 0)

    def ring_copy(step, p):
        return remote(
            ring_out.at[step - 1, :, piece_of(p)],
            ring_in.at[step - 1, :, piece_of(p)],
            ring_send.at[step - 1],
            ring_recv.at[step - 1, p],
            "ep",
            group_of(step, core),
        )

    @pl.when(core != FIRST)
    def _():
        give()
        pl.semaphore_wait(gate, 1)

    shares = [share_of(group_of(step, core)) for step in range(ring)]
    order = sorted(range(1, ring), key=lambda step: abs(2 * step - ring))

    def scale_copy(step, p):
        return remote(
            scale_out.at[step - 1, p],
            scale_in.at[step - 1, p],
            scale_send.at[step - 1],
            scale_recv.at[step - 1, p],
            "ep",
            group_of(step, core),
        )

    def spread_lanes(row, width):
        return jnp.concatenate([row] * (width // LANES), axis=1)

    def send_piece(p, carry):
        pair_copy(p).wait_recv()
        cols = piece_of(p)
        for step in order:
            total = weighted(shares[step], core, step, cols).astype(jnp.float32)
            total = total + pair_in[step, :, cols].astype(jnp.float32)
            most = jnp.max(jnp.abs(total), axis=0, keepdims=True)
            parts = [most[:, j : j + LANES] for j in range(0, piece, LANES)]
            most = jnp.maximum(functools.reduce(jnp.maximum, parts), TINY)
            scale_out[step - 1, p] = most * (1.0 / CODES)
            codes = lax.round(
                total * spread_lanes(CODES / most, piece), lax.RoundingMethod.TO_NEAREST_EVEN
            )
            ring_out[step - 1, :, cols] = codes.astype(jnp.int32).astype(jnp.int16)
            ring_copy(step, p).start()
            scale_copy(step, p).start()
        return carry

    lax.fori_loop(0, pieces, send_piece, 0)

    @pl.when(core == FIRST)
    def _():
        give()

    shape = (rows, layer.shape[1])
    lane = lax.broadcasted_iota(jnp.int32, shape, 1)
    slot = lane // rows
    diagonal = lane % rows == lax.broadcasted_iota(jnp.int32, shape, 0)

    def halves(value):
        high = value.astype(jnp.bfloat16).astype(jnp.float32)
        return high, value - high

    def place(h, carry):
        block = jnp.zeros(shape, jnp.float32)
        for f in range(5):
            high, low = halves(jnp.full(shape, in_weight[f, h]))
            whole = slot == f
            if f < 4:
                whole = jnp.logical_or(whole, slot == 5 + f)
            block = jnp.where(whole, high, jnp.where(slot == 9 + f, low, block))
        block = jnp.where(diagonal, block, 0.0)
        layer[pl.ds(pl.multiple_of(h * rows, rows), rows), :] = block.astype(jnp.bfloat16)
        return carry

    lax.fori_loop(0, units, place, 0)
    for copy in params:
        copy.wait()

    def moments(p, carry):
        for step in range(1, ring):
            ring_copy(step, p).wait_recv()
            scale_copy(step, p).wait_recv()
        scales = [
            spread_lanes(scale_in[step - 1, p], narrow) for step in range(1, ring)
        ]

        @pl.when(jnp.logical_and(core == FIRST, p == GATE_PIECE))
        def _():
            pl.semaphore_signal(
                gate,
                inc=1,
                device_id={"ep": partner},
                device_id_type=pl.DeviceIdType.MESH,
            )

        def one(i, inner):
            grad_acc, mom_acc = inner
            cols = cols_of(p, i)
            total = weighted(shares[0], core, 0, cols).astype(jnp.float32)
            total = total + pair_in[0, :, cols].astype(jnp.float32)
            for step in range(1, ring):
                codes = ring_in[step - 1, :, cols].astype(jnp.int32).astype(jnp.float32)
                total = total + codes * scales[step - 1]
            mom_next = MOMENTUM_DECAY * mom[:, cols] + (1.0 - MOMENTUM_DECAY) * total
            gradient[:, cols] = total
            mom[:, cols] = mom_next
            second[:, cols] = (
                SECOND_DECAY * second[:, cols] + (1.0 - SECOND_DECAY) * total * total
            )
            return grad_acc + total * total, mom_acc + mom_next * mom_next

        return lax.fori_loop(0, piece // narrow, one, carry)

    zero = jnp.zeros((rows, narrow), jnp.float32)
    grad_acc, mom_acc = lax.fori_loop(0, pieces, moments, (zero, zero))

    def to_lanes(acc):
        acc = jnp.sum(acc, axis=0, keepdims=True)
        return sum(acc[:, j : j + LANES] for j in range(0, narrow, LANES))

    sums[me, 0:1, :] = to_lanes(grad_acc)
    sums[me, 1:2, :] = to_lanes(mom_acc)
    for step in range(1, shards):
        remote(
            sums.at[me], sums.at[me], sum_send, sum_recv, "fs", (me + step) % shards
        ).start()
    others = sums.at[pl.ds(0, shards - 1)]
    all_sums = remote(others, others, sum_send, sum_recv, "fs", (me + 1) % shards)
    all_sums.wait_recv()

    entries = rows * columns * shards
    totals = sums[0]
    for s in range(1, shards):
        totals = totals + sums[s]
    mean = jnp.broadcast_to(jnp.sum(totals, axis=1, keepdims=True) / entries, (2, LANES)) + NORM_EPS
    inverse = lax.rsqrt(mean)
    inv_grad = inverse[0:1, :1]
    inv_mom = inverse[1:2, :1]
    log_mom = jnp.max(0.5 * jnp.log(mean[1:2, :]))
    tail = pl.ds(shape[1] - LANES, LANES)
    biased = slot[:, -LANES:] >= 14
    first = slot[:, -LANES:] == 14
    ends = diagonal[:, -LANES:]

    def settle(h, carry):
        high, low = halves(jnp.full(ends.shape, in_bias[h] + in_weight[5, h] * log_mom))
        span = pl.ds(pl.multiple_of(h * rows, rows), rows)
        block = jnp.where(ends, jnp.where(first, high, low), 0.0)
        kept = layer[span, tail].astype(jnp.float32)
        layer[span, tail] = jnp.where(biased, block, kept).astype(jnp.bfloat16)
        return carry

    lax.fori_loop(0, units, settle, 0)

    chunks = pass_recv.shape[1]
    width = columns // chunks
    tile = tile_width(width, TILE)

    def learned_step(cols):
        grad = gradient[:, cols]
        mom_next = mom[:, cols]
        narrow_old = weight[:, cols]
        inv_root = lax.rsqrt(second[:, cols] + ROOT_EPS)
        highs, lows = [], []
        for value in (
            grad * inv_grad,
            mom_next * inv_mom,
            mom_next * inv_root,
            grad * inv_root,
        ):
            high = value.astype(jnp.bfloat16)
            highs.append(high)
            lows.append((value - high.astype(jnp.float32)).astype(jnp.bfloat16))
        highs.append(narrow_old)
        ones = jnp.ones(grad.shape, jnp.bfloat16)
        features = jnp.concatenate(highs + lows + highs + [ones, ones], axis=0)
        hidden = jnp.dot(layer[...], features, preferred_element_type=jnp.float32)
        directions = [jnp.full(grad.shape, out_bias[0]), jnp.zeros(grad.shape, jnp.float32)]
        magnitudes = [jnp.full(grad.shape, out_bias[1]), jnp.zeros(grad.shape, jnp.float32)]
        for h in range(units):
            active = jnp.maximum(hidden[h * rows : (h + 1) * rows, :], 0.0)
            side = 2 * h // units
            directions[side] = directions[side] + active * out_weight[0, h]
            magnitudes[side] = magnitudes[side] + active * out_weight[1, h]
        direction = directions[0] + directions[1]
        magnitude = magnitudes[0] + magnitudes[1]
        update = STEP_SCALE * direction * jnp.exp(EXP_SCALE * magnitude)
        return (narrow_old.astype(jnp.float32) - update).astype(jnp.bfloat16)

    def rows_of(source):
        return pl.ds(pl.multiple_of(source * rows, rows), rows)

    def block(source, k):
        return gathered.at[rows_of(source), pl.ds(pl.multiple_of(k * width, width), width)]

    def route(k):
        swap = k % 2
        turn = 1 - 2 * (k // 2 % 2)

        def at(first, after):
            up = (z + 2 * SIDE + first * swap + after * (1 - swap)) % SIDE
            along = (x + 2 * SIDE + first * (1 - swap) + after * swap) % SIDE
            return up * SIDE + along

        return at, turn

    def send(source, k, role, recv, peer):
        remote(block(source, k), block(source, k), row_send.at[role], recv, "fs", peer).start()

    def spread(source, k, role, part, at, way):
        send(source, k, role, pass_recv.at[part, k], at(0, way))
        send(source, k, role, last_recv.at[source], at(0, -way))

    def arrive(source, k, part):
        remote(
            block(source, k), block(source, k), row_send.at[0], pass_recv.at[part, k], "fs", source
        ).wait_recv()

    def own(k):
        at, turn = route(k)
        send(me, k, 0, pass_recv.at[0, k], at(turn, 0))
        send(me, k, 0, pass_recv.at[1, k], at(-turn, 0))
        spread(me, k, 0, 3, at, turn)

    def pass_on(k, role, first, part):
        at, turn = route(k)
        way = turn if first % 2 == 0 else -turn
        source = at(first * turn, -way)
        arrive(source, k, part)
        send(source, k, role, last_recv.at[source], at(0, way))

    def relay_one(k):
        at, turn = route(k)
        source = at(-turn, 0)
        arrive(source, k, 0)
        send(source, k, 1, pass_recv.at[2, k], at(turn, 0))
        spread(source, k, 1, 4, at, -turn)
        source = at(turn, 0)
        arrive(source, k, 1)
        spread(source, k, 1, 5, at, -turn)
        pass_on(k, 1, 0, 3)

    def relay_two(k):
        at, turn = route(k)
        source = at(2, 0)
        arrive(source, k, 2)
        spread(source, k, 2, 6, at, turn)
        pass_on(k, 2, -1, 4)
        pass_on(k, 2, 1, 5)

    def relay_three(k):
        pass_on(k, 3, 2, 6)

    def turn_of(t, carry):
        for lag, relay in ((LAG_ONE, relay_one), (LAG_TWO, relay_two), (LAG_THREE, relay_three)):
            k = t - lag

            @pl.when(jnp.logical_and(k >= 0, k < chunks))
            def _(k=k, relay=relay):
                relay(k)

        @pl.when(t < chunks)
        def _():
            def one(i, inner):
                cols = pl.ds(pl.multiple_of(t * width + i * tile, tile), tile)
                gathered[rows_of(me), cols] = learned_step(cols)
                return inner

            lax.fori_loop(0, width // tile, one, 0)
            own(t)

        return carry

    lax.fori_loop(0, chunks + LAG_THREE, turn_of, 0)

    remote(pair_out, pair_in, pair_send, pair_recv.at[0], "ep", partner).wait_send()
    for step in range(1, ring):
        remote(
            ring_out.at[step - 1],
            ring_in.at[step - 1],
            ring_send.at[step - 1],
            ring_recv.at[step - 1, 0],
            "ep",
            group_of(step, core),
        ).wait_send()
        remote(
            scale_out.at[step - 1],
            scale_in.at[step - 1],
            scale_send.at[step - 1],
            scale_recv.at[step - 1, 0],
            "ep",
            group_of(step, core),
        ).wait_send()
    all_sums.wait_send()
    share = {0: 0, 1: chunks // 4, 2: chunks // 2, 3: chunks // 4}
    for up in range(SIDE):
        for along in range(SIDE):
            number = share[up] + share[along]
            if number == 0:
                continue
            source = (z + up) % SIDE * SIDE + (x + along) % SIDE
            part = gathered.at[rows_of(source), pl.ds(0, number * width)]
            remote(part, part, row_send.at[0], last_recv.at[source], "fs", source).wait_recv()
    for role, number in enumerate((4, 6, 4, 1)):
        part = gathered.at[pl.ds(0, number * rows), :]
        remote(
            part, part, row_send.at[role], last_recv.at[me], "fs", (me + 1) % shards
        ).wait_send()


def store(gathered, mom, second, gathered_hbm, mom_hbm, second_hbm, sems):
    height = gathered.shape[1] // STORES
    copies = [
        pltpu.make_async_copy(
            gathered.at[:, pl.ds(i * height, height), :],
            gathered_hbm.at[:, pl.ds(i * height, height), :],
            sems.at[i],
        )
        for i in range(STORES)
    ]
    copies.append(pltpu.make_async_copy(mom, mom_hbm, sems.at[STORES]))
    copies.append(pltpu.make_async_copy(second, second_hbm, sems.at[STORES + 1]))
    for copy in copies:
        copy.start()
    for copy in copies:
        copy.wait()


def per_device(groups, grads, counts, weight, mom, second, in_weight, in_bias, out_weight, out_bias):
    rows, columns = mom.shape[1], mom.shape[2]
    ring = groups // CORES
    shards = SIDE * SIDE
    pieces = PIECES
    chunks = CHUNKS
    hbm = pl.BlockSpec(memory_space=pltpu.HBM)
    vmem = pl.BlockSpec(memory_space=pltpu.VMEM)
    results = pl.pallas_call(
        functools.partial(kernel, ring),
        out_shape=(
            pltpu.VMEM((1, rows * shards, columns), jnp.bfloat16),
            pltpu.VMEM(mom.shape, jnp.float32),
            pltpu.VMEM(second.shape, jnp.float32),
        ),
        in_specs=[hbm] * 9,
        out_specs=(vmem, vmem, vmem),
        scratch_shapes=[
            pltpu.SMEM(counts.shape, jnp.int32),
            pltpu.SMEM(in_weight.shape, jnp.float32),
            pltpu.SMEM(in_bias.shape, jnp.float32),
            pltpu.SMEM(out_weight.shape[::-1], jnp.float32),
            pltpu.SMEM(out_bias.shape, jnp.float32),
            pltpu.VMEM((CORES, ring, rows, columns), jnp.bfloat16),
            pltpu.VMEM((rows, columns), jnp.bfloat16),
            pltpu.VMEM((ring, rows, columns), jnp.bfloat16),
            pltpu.VMEM((ring, rows, columns), jnp.bfloat16),
            pltpu.VMEM((ring - 1, rows, columns), jnp.int16),
            pltpu.VMEM((ring - 1, rows, columns), jnp.int16),
            pltpu.VMEM((ring - 1, pieces, 1, LANES), jnp.float32),
            pltpu.VMEM((ring - 1, pieces, 1, LANES), jnp.float32),
            pltpu.VMEM((rows, columns), jnp.float32),
            pltpu.VMEM((shards, 2, LANES), jnp.float32),
            pltpu.VMEM((in_bias.shape[0] * rows, 16 * rows), jnp.bfloat16),
            pltpu.SemaphoreType.DMA((5,)),
            pltpu.SemaphoreType.DMA((CORES, ring)),
            pltpu.SemaphoreType.DMA((3,)),
            pltpu.SemaphoreType.DMA,
            pltpu.SemaphoreType.DMA((pieces,)),
            pltpu.SemaphoreType.DMA((ring - 1,)),
            pltpu.SemaphoreType.DMA((ring - 1, pieces)),
            pltpu.SemaphoreType.DMA((ring - 1,)),
            pltpu.SemaphoreType.DMA((ring - 1, pieces)),
            pltpu.SemaphoreType.REGULAR,
            pltpu.SemaphoreType.DMA,
            pltpu.SemaphoreType.DMA,
            pltpu.SemaphoreType.DMA((4,)),
            pltpu.SemaphoreType.DMA((7, chunks)),
            pltpu.SemaphoreType.DMA((shards,)),
        ],
        compiler_params=pltpu.CompilerParams(
            collective_id=0, has_side_effects=True, vmem_limit_bytes=VMEM_BYTES
        ),
        name="learned_update",
    )(counts, in_weight, in_bias, out_weight.T, out_bias, grads, weight, mom, second)
    return pl.pallas_call(
        store,
        out_shape=[jax.ShapeDtypeStruct(r.shape, r.dtype) for r in results],
        in_specs=[vmem] * 3,
        out_specs=[hbm] * 3,
        scratch_shapes=[pltpu.SemaphoreType.DMA((STORES + 2,))],
        compiler_params=pltpu.CompilerParams(vmem_limit_bytes=1024 * 1024),
        name="store_results",
    )(*results)


def solution(mesh):
    in_specs = (
        P("ep", None, "fs", None),
        P(),
        P("ep", "fs", None),
        P("ep", "fs", None),
        P("ep", "fs", None),
        P(),
        P(),
        P(),
        P(),
    )
    out_specs = (P("ep", None, None), P("ep", "fs", None), P("ep", "fs", None))
    body = functools.partial(per_device, mesh.shape["ep"])
    return jax.shard_map(
        body, mesh=mesh, in_specs=in_specs, out_specs=out_specs, check_vma=False
    )
```

```python
import functools

import jax
import jax.numpy as jnp
from jax import lax
from jax.experimental import pallas as pl
from jax.experimental.pallas import tpu as pltpu
from jax.sharding import PartitionSpec as P

MOMENTUM_DECAY = 0.9
SECOND_DECAY = 0.99
NORM_EPS = 1e-06
ROOT_EPS = 1e-08
STEP_SCALE = 0.2
EXP_SCALE = 0.5
LANES = 128
CORES = 2
SIDE = 4
CHUNKS = 16
PIECES = 8
LAG_ONE = 6
LAG_TWO = 11
LAG_THREE = 16
GATE_PIECE = 6
FIRST = 1
ORDER = (2, 1, 3, 0)
CODES = 32767.0
TINY = 1e-30
TILE = 896
STORES = 4
VMEM_BYTES = 67043328 - 9175040


def largest_divisor(number, most):
    return max(d for d in range(1, most + 1) if number % d == 0)


def tile_width(columns, most):
    return LANES * largest_divisor(columns // LANES, most // LANES)


def remote(src, dst, send_sem, recv_sem, axis, peer):
    return pltpu.make_async_remote_copy(
        src_ref=src,
        dst_ref=dst,
        send_sem=send_sem,
        recv_sem=recv_sem,
        device_id={axis: peer},
        device_id_type=pl.DeviceIdType.MESH,
    )


def kernel(
    ring,
    counts_hbm,
    in_weight_hbm,
    in_bias_hbm,
    out_weight_hbm,
    out_bias_hbm,
    grads_hbm,
    weight_hbm,
    mom_hbm,
    second_hbm,
    gathered_out,
    mom_out,
    second_out,
    counts,
    in_weight,
    in_bias,
    out_weight,
    out_bias,
    grads,
    weight,
    pair_out,
    pair_in,
    ring_out,
    ring_in,
    scale_out,
    scale_in,
    gradient,
    sums,
    layer,
    tally,
    small_sem,
    slab_sem,
    param_sem,
    pair_send,
    pair_recv,
    ring_send,
    ring_recv,
    scale_send,
    gate,
    sum_send,
    sum_recv,
    row_send,
    pass_recv,
    last_recv,
):
    gathered = gathered_out.at[0]
    mom = mom_out.at[0]
    second = second_out.at[0]
    groups = ring * CORES
    shards = SIDE * SIDE
    rows, columns = gradient.shape
    units = in_bias.shape[0]
    me_group = lax.axis_index("ep")
    me = lax.axis_index("fs")
    y = me_group // CORES
    core = me_group % CORES
    partner = y * CORES + 1 - core
    z = me // SIDE
    x = me % SIDE

    def group_of(step, which):
        return (y + step) % ring * CORES + which

    small = [
        pltpu.make_async_copy(src, dst, small_sem.at[i])
        for i, (src, dst) in enumerate(
            (
                (counts_hbm, counts),
                (in_weight_hbm, in_weight),
                (in_bias_hbm, in_bias),
                (out_weight_hbm, out_weight),
                (out_bias_hbm, out_bias),
            )
        )
    ]
    for copy in small:
        copy.start()

    def slab(which, step):
        return pltpu.make_async_copy(
            grads_hbm.at[0, group_of(step, which)],
            grads.at[which, step],
            slab_sem.at[which],
        )

    def slabs_in(which):
        pltpu.make_async_copy(
            grads_hbm.at[0, pl.ds(0, ring)], grads.at[which], slab_sem.at[which]
        ).wait()

    for which in (FIRST, 1 - FIRST):
        for step in ORDER:
            slab(which, step).start()
    barrier = pltpu.get_barrier_semaphore()
    for peer in [partner] + [group_of(step, core) for step in range(1, ring)]:
        pl.semaphore_signal(
            barrier, inc=1, device_id={"ep": peer}, device_id_type=pl.DeviceIdType.MESH
        )
    for step in range(1, shards):
        pl.semaphore_signal(
            barrier,
            inc=1,
            device_id={"fs": (me + step) % shards},
            device_id_type=pl.DeviceIdType.MESH,
        )
    small[0].wait()

    pieces = ring_recv.shape[1]
    piece = columns // pieces
    narrow = tile_width(piece, 512)

    def cols_of(p, i):
        return pl.ds(pl.multiple_of(p * piece + i * narrow, narrow), narrow)

    def piece_of(p):
        return pl.ds(pl.multiple_of(p * piece, piece), piece)

    def share_of(expert):
        total = counts[0, expert]
        for s in range(1, groups):
            total = total + counts[s, expert]
        mine = jnp.full((1, LANES), counts[me_group, expert].astype(jnp.float32))
        return (mine / jnp.full((1, LANES), total.astype(jnp.float32)))[:, :1]

    def weighted(share, which, step, cols):
        value = share * grads[which, step, :, cols].astype(jnp.float32)
        return value.astype(jnp.bfloat16)

    slabs_in(FIRST)
    pl.semaphore_wait(barrier, 1 + ring - 1 + shards - 1)

    def pair_copy(part, p):
        slots = (pl.ds(0, 1), pl.ds(1, ring - 1))[part]
        return remote(
            pair_out.at[slots, :, piece_of(p)],
            pair_in.at[slots, :, piece_of(p)],
            pair_send.at[part],
            pair_recv.at[part, p],
            "ep",
            partner,
        )

    def give():
        shares = [share_of(group_of(step, 1 - core)) for step in range(ring)]
        for part, steps in enumerate((ORDER[:1], ORDER[1:])):

            def body(p, carry, part=part, steps=steps):
                for step in steps:
                    pair_out[ORDER.index(step), :, piece_of(p)] = weighted(
                        shares[step], 1 - core, step, piece_of(p)
                    )
                pair_copy(part, p).start()
                return carry

            lax.fori_loop(0, pieces, body, 0)

    def hop(slot, p, odd=0):
        step = (1 - 2 * odd, 1, -1)[slot]
        peer = group_of(step + ring, core)
        codes = remote(
            ring_out.at[slot, :, piece_of(p)],
            ring_in.at[slot, :, piece_of(p)],
            ring_send.at[slot],
            ring_recv.at[slot, p],
            "ep",
            peer,
        )
        scale = remote(
            scale_out.at[slot, p],
            scale_in.at[slot, p],
            scale_send.at[slot],
            ring_recv.at[slot, p],
            "ep",
            peer,
        )
        return codes, scale

    def landed(slot, p):
        remote(tally, tally, ring_send.at[slot], ring_recv.at[slot, p], "ep", partner).wait_recv()

    def spread_lanes(row, width):
        return jnp.concatenate([row] * (width // LANES), axis=1)

    def pair_sum(step, cols):
        total = weighted(shares[step], core, step, cols).astype(jnp.float32)
        return total + pair_in[ORDER.index(step), :, cols].astype(jnp.float32)

    def decode(slot, p, cols, width):
        codes = ring_in[slot, :, cols].astype(jnp.int32).astype(jnp.float32)
        return codes * spread_lanes(scale_in[slot, p], width)

    def encode(slot, p, odd, total):
        most = jnp.max(jnp.abs(total), axis=0, keepdims=True)
        parts = [most[:, j : j + LANES] for j in range(0, piece, LANES)]
        most = jnp.maximum(functools.reduce(jnp.maximum, parts), TINY)
        scale_out[slot, p] = most * (1.0 / CODES)
        codes = lax.round(
            total * spread_lanes(CODES / most, piece), lax.RoundingMethod.TO_NEAREST_EVEN
        )
        ring_out[slot, :, piece_of(p)] = codes.astype(jnp.int32).astype(jnp.int16)
        for copy in hop(slot, p, odd):
            copy.start()

    @pl.when(core != FIRST)
    def _():
        give()
        pl.semaphore_wait(gate, 1)

    shares = [share_of(group_of(step, core)) for step in range(ring)]
    @pl.when(core != FIRST)
    def _():
        slabs_in(1 - FIRST)

    def far(q, carry):
        for odd in range(2):
            p = 2 * q + odd
            pair_copy(0, p).wait_recv()
            encode(0, p, odd, pair_sum(2, piece_of(p)))
        return carry

    lax.fori_loop(0, pieces // 2, far, 0)

    def near(q, carry):
        for odd in range(2):
            p = 2 * q + odd
            pair_copy(1, p).wait_recv()
            slot, step = ((2, 3), (1, 1))[odd]
            encode(slot, p, odd, pair_sum(step, piece_of(p)))
            slot, step = ((1, 1), (2, 3))[odd]
            landed(0, p)
            encode(slot, p, odd, pair_sum(step, piece_of(p)) + decode(0, p, piece_of(p), piece))
        return carry

    lax.fori_loop(0, pieces // 2, near, 0)

    @pl.when(core == FIRST)
    def _():
        slabs_in(1 - FIRST)
        give()

    for copy in small[1:]:
        copy.wait()
    params = [
        pltpu.make_async_copy(src.at[0], dst, param_sem.at[i])
        for i, (src, dst) in enumerate(
            ((mom_hbm, mom), (second_hbm, second), (weight_hbm, weight))
        )
    ]
    for copy in params:
        copy.start()


    shape = (rows, layer.shape[1])
    lane = lax.broadcasted_iota(jnp.int32, shape, 1)
    slot = lane // rows
    diagonal = lane % rows == lax.broadcasted_iota(jnp.int32, shape, 0)

    def halves(value):
        high = value.astype(jnp.bfloat16).astype(jnp.float32)
        return high, value - high

    def place(h, carry):
        block = jnp.zeros(shape, jnp.float32)
        for f in range(5):
            high, low = halves(jnp.full(shape, in_weight[f, h]))
            whole = slot == f
            if f < 4:
                whole = jnp.logical_or(whole, slot == 5 + f)
            block = jnp.where(whole, high, jnp.where(slot == 9 + f, low, block))
        block = jnp.where(diagonal, block, 0.0)
        layer[pl.ds(pl.multiple_of(h * rows, rows), rows), :] = block.astype(jnp.bfloat16)
        return carry

    lax.fori_loop(0, units, place, 0)
    for copy in params:
        copy.wait()

    def moments(p, carry):
        for slot in (1, 2):
            landed(slot, p)

        @pl.when(jnp.logical_and(core == FIRST, p == GATE_PIECE))
        def _():
            pl.semaphore_signal(
                gate,
                inc=1,
                device_id={"ep": partner},
                device_id_type=pl.DeviceIdType.MESH,
            )

        def one(i, inner):
            grad_acc, mom_acc = inner
            cols = cols_of(p, i)
            total = pair_sum(0, cols) + decode(1, p, cols, narrow) + decode(2, p, cols, narrow)
            mom_next = MOMENTUM_DECAY * mom[:, cols] + (1.0 - MOMENTUM_DECAY) * total
            gradient[:, cols] = total
            mom[:, cols] = mom_next
            second[:, cols] = (
                SECOND_DECAY * second[:, cols] + (1.0 - SECOND_DECAY) * total * total
            )
            return grad_acc + total * total, mom_acc + mom_next * mom_next

        return lax.fori_loop(0, piece // narrow, one, carry, unroll=True)

    zero = jnp.zeros((rows, narrow), jnp.float32)
    grad_acc, mom_acc = lax.fori_loop(0, pieces, moments, (zero, zero))

    def to_lanes(acc):
        acc = jnp.sum(acc, axis=0, keepdims=True)
        return sum(acc[:, j : j + LANES] for j in range(0, narrow, LANES))

    sums[me, 0:1, :] = to_lanes(grad_acc)
    sums[me, 1:2, :] = to_lanes(mom_acc)
    for step in range(1, shards):
        remote(
            sums.at[me], sums.at[me], sum_send, sum_recv, "fs", (me + step) % shards
        ).start()
    others = sums.at[pl.ds(0, shards - 1)]
    all_sums = remote(others, others, sum_send, sum_recv, "fs", (me + 1) % shards)
    all_sums.wait_recv()

    entries = rows * columns * shards
    totals = sums[0]
    for s in range(1, shards):
        totals = totals + sums[s]
    mean = jnp.broadcast_to(jnp.sum(totals, axis=1, keepdims=True) / entries, (2, LANES)) + NORM_EPS
    inverse = lax.rsqrt(mean)
    inv_grad = inverse[0:1, :1]
    inv_mom = inverse[1:2, :1]
    log_mom = jnp.max(0.5 * jnp.log(mean[1:2, :]))
    tail = pl.ds(shape[1] - LANES, LANES)
    biased = slot[:, -LANES:] >= 14
    first = slot[:, -LANES:] == 14
    ends = diagonal[:, -LANES:]

    def settle(h, carry):
        high, low = halves(jnp.full(ends.shape, in_bias[h] + in_weight[5, h] * log_mom))
        span = pl.ds(pl.multiple_of(h * rows, rows), rows)
        block = jnp.where(ends, jnp.where(first, high, low), 0.0)
        kept = layer[span, tail].astype(jnp.float32)
        layer[span, tail] = jnp.where(biased, block, kept).astype(jnp.bfloat16)
        return carry

    lax.fori_loop(0, units, settle, 0)

    chunks = pass_recv.shape[1]
    width = columns // chunks
    tile = tile_width(width, TILE)

    def learned_step(cols):
        grad = gradient[:, cols]
        mom_next = mom[:, cols]
        narrow_old = weight[:, cols]
        inv_root = lax.rsqrt(second[:, cols] + ROOT_EPS)
        highs, lows = [], []
        for value in (
            grad * inv_grad,
            mom_next * inv_mom,
            mom_next * inv_root,
            grad * inv_root,
        ):
            high = value.astype(jnp.bfloat16)
            highs.append(high)
            lows.append((value - high.astype(jnp.float32)).astype(jnp.bfloat16))
        highs.append(narrow_old)
        ones = jnp.ones(grad.shape, jnp.bfloat16)
        features = jnp.concatenate(highs + lows + highs + [ones, ones], axis=0)
        hidden = jnp.dot(layer[...], features, preferred_element_type=jnp.float32)
        directions = [jnp.full(grad.shape, out_bias[0]), jnp.zeros(grad.shape, jnp.float32)]
        magnitudes = [jnp.full(grad.shape, out_bias[1]), jnp.zeros(grad.shape, jnp.float32)]
        for h in range(units):
            active = jnp.maximum(hidden[h * rows : (h + 1) * rows, :], 0.0)
            side = 2 * h // units
            directions[side] = directions[side] + active * out_weight[0, h]
            magnitudes[side] = magnitudes[side] + active * out_weight[1, h]
        direction = directions[0] + directions[1]
        magnitude = magnitudes[0] + magnitudes[1]
        update = STEP_SCALE * direction * jnp.exp(EXP_SCALE * magnitude)
        return (narrow_old.astype(jnp.float32) - update).astype(jnp.bfloat16)

    def rows_of(source):
        return pl.ds(pl.multiple_of(source * rows, rows), rows)

    def block(source, k):
        return gathered.at[rows_of(source), pl.ds(pl.multiple_of(k * width, width), width)]

    def route(k):
        swap = k % 2
        turn = 1 - 2 * (k // 2 % 2)

        def at(first, after):
            up = (z + 2 * SIDE + first * swap + after * (1 - swap)) % SIDE
            along = (x + 2 * SIDE + first * (1 - swap) + after * swap) % SIDE
            return up * SIDE + along

        return at, turn

    def send(source, k, role, recv, peer):
        remote(block(source, k), block(source, k), row_send.at[role], recv, "fs", peer).start()

    def spread(source, k, role, at, way):
        send(source, k, role, pass_recv.at[role, k], at(0, way))
        send(source, k, role, last_recv.at[source], at(0, -way))

    def arrive(stage, k, count):
        part = gathered.at[pl.ds(0, count * rows), pl.ds(pl.multiple_of(k * width, width), width)]
        remote(part, part, row_send.at[0], pass_recv.at[stage, k], "fs", me).wait_recv()

    def pass_on(k, role, first):
        at, turn = route(k)
        way = turn if first % 2 == 0 else -turn
        source = at(first * turn, -way)
        send(source, k, role, last_recv.at[source], at(0, way))

    def own(k):
        at, turn = route(k)
        send(me, k, 0, pass_recv.at[0, k], at(turn, 0))
        send(me, k, 0, pass_recv.at[0, k], at(-turn, 0))
        spread(me, k, 0, at, turn)

    def relay_one(k):
        at, turn = route(k)
        arrive(0, k, 3)
        source = at(-turn, 0)
        send(source, k, 1, pass_recv.at[1, k], at(turn, 0))
        spread(source, k, 1, at, -turn)
        spread(at(turn, 0), k, 1, at, -turn)
        pass_on(k, 1, 0)

    def relay_two(k):
        at, turn = route(k)
        arrive(1, k, 3)
        spread(at(2, 0), k, 2, at, turn)
        pass_on(k, 2, -1)
        pass_on(k, 2, 1)

    def relay_three(k):
        arrive(2, k, 1)
        pass_on(k, 3, 2)

    def turn_of(t, carry):
        for lag, relay in ((LAG_ONE, relay_one), (LAG_TWO, relay_two), (LAG_THREE, relay_three)):
            k = t - lag

            @pl.when(jnp.logical_and(k >= 0, k < chunks))
            def _(k=k, relay=relay):
                relay(k)

        @pl.when(t < chunks)
        def _():
            def one(i, inner):
                cols = pl.ds(pl.multiple_of(t * width + i * tile, tile), tile)
                gathered[rows_of(me), cols] = learned_step(cols)
                return inner

            lax.fori_loop(0, width // tile, one, 0)
            own(t)

        return carry

    lax.fori_loop(0, chunks + LAG_THREE, turn_of, 0)

    for part in range(2):
        slots = (pl.ds(0, 1), pl.ds(1, ring - 1))[part]
        remote(
            pair_out.at[slots], pair_in.at[slots], pair_send.at[part], pair_recv.at[part, 0], "ep", partner
        ).wait_send()
    for slot in range(3):
        remote(
            ring_out.at[slot], ring_in.at[slot], ring_send.at[slot], ring_recv.at[slot, 0], "ep", partner
        ).wait_send()
        remote(
            scale_out.at[slot], scale_in.at[slot], scale_send.at[slot], ring_recv.at[slot, 0], "ep", partner
        ).wait_send()
    all_sums.wait_send()
    share = {0: 0, 1: chunks // 4, 2: chunks // 2, 3: chunks // 4}
    for up in range(SIDE):
        for along in range(SIDE):
            number = share[up] + share[along]
            if number == 0:
                continue
            source = (z + up) % SIDE * SIDE + (x + along) % SIDE
            part = gathered.at[rows_of(source), pl.ds(0, number * width)]
            remote(part, part, row_send.at[0], last_recv.at[source], "fs", source).wait_recv()
    for role, number in enumerate((4, 6, 4, 1)):
        part = gathered.at[pl.ds(0, number * rows), :]
        remote(
            part, part, row_send.at[role], last_recv.at[me], "fs", (me + 1) % shards
        ).wait_send()


def store(gathered, mom, second, gathered_hbm, mom_hbm, second_hbm, sems):
    height = gathered.shape[1] // STORES
    copies = [
        pltpu.make_async_copy(
            gathered.at[:, pl.ds(i * height, height), :],
            gathered_hbm.at[:, pl.ds(i * height, height), :],
            sems.at[i],
        )
        for i in range(STORES)
    ]
    copies.append(pltpu.make_async_copy(mom, mom_hbm, sems.at[STORES]))
    copies.append(pltpu.make_async_copy(second, second_hbm, sems.at[STORES + 1]))
    for copy in copies:
        copy.start()
    for copy in copies:
        copy.wait()


def per_device(groups, grads, counts, weight, mom, second, in_weight, in_bias, out_weight, out_bias):
    rows, columns = mom.shape[1], mom.shape[2]
    ring = groups // CORES
    shards = SIDE * SIDE
    pieces = PIECES
    chunks = CHUNKS
    hbm = pl.BlockSpec(memory_space=pltpu.HBM)
    vmem = pl.BlockSpec(memory_space=pltpu.VMEM)
    results = pl.pallas_call(
        functools.partial(kernel, ring),
        out_shape=(
            pltpu.VMEM((1, rows * shards, columns), jnp.bfloat16),
            pltpu.VMEM(mom.shape, jnp.float32),
            pltpu.VMEM(second.shape, jnp.float32),
        ),
        in_specs=[hbm] * 9,
        out_specs=(vmem, vmem, vmem),
        scratch_shapes=[
            pltpu.SMEM(counts.shape, jnp.int32),
            pltpu.SMEM(in_weight.shape, jnp.float32),
            pltpu.SMEM(in_bias.shape, jnp.float32),
            pltpu.SMEM(out_weight.shape[::-1], jnp.float32),
            pltpu.SMEM(out_bias.shape, jnp.float32),
            pltpu.VMEM((CORES, ring, rows, columns), jnp.bfloat16),
            pltpu.VMEM((rows, columns), jnp.bfloat16),
            pltpu.VMEM((ring, rows, columns), jnp.bfloat16),
            pltpu.VMEM((ring, rows, columns), jnp.bfloat16),
            pltpu.VMEM((ring - 1, rows, columns), jnp.int16),
            pltpu.VMEM((ring - 1, rows, columns), jnp.int16),
            pltpu.VMEM((ring - 1, pieces, 1, LANES), jnp.float32),
            pltpu.VMEM((ring - 1, pieces, 1, LANES), jnp.float32),
            pltpu.VMEM((rows, columns), jnp.float32),
            pltpu.VMEM((shards, 2, LANES), jnp.float32),
            pltpu.VMEM((in_bias.shape[0] * rows, 16 * rows), jnp.bfloat16),
            pltpu.VMEM((rows * columns // pieces * 2 // (4 * LANES) + 1, LANES), jnp.float32),
            pltpu.SemaphoreType.DMA((5,)),
            pltpu.SemaphoreType.DMA((CORES,)),
            pltpu.SemaphoreType.DMA((3,)),
            pltpu.SemaphoreType.DMA((2,)),
            pltpu.SemaphoreType.DMA((2, pieces)),
            pltpu.SemaphoreType.DMA((ring - 1,)),
            pltpu.SemaphoreType.DMA((ring - 1, pieces)),
            pltpu.SemaphoreType.DMA((ring - 1,)),
            pltpu.SemaphoreType.REGULAR,
            pltpu.SemaphoreType.DMA,
            pltpu.SemaphoreType.DMA,
            pltpu.SemaphoreType.DMA((4,)),
            pltpu.SemaphoreType.DMA((3, chunks)),
            pltpu.SemaphoreType.DMA((shards,)),
        ],
        compiler_params=pltpu.CompilerParams(
            collective_id=0, has_side_effects=True, vmem_limit_bytes=VMEM_BYTES
        ),
        name="learned_update",
    )(counts, in_weight, in_bias, out_weight.T, out_bias, grads, weight, mom, second)
    return pl.pallas_call(
        store,
        out_shape=[jax.ShapeDtypeStruct(r.shape, r.dtype) for r in results],
        in_specs=[vmem] * 3,
        out_specs=[hbm] * 3,
        scratch_shapes=[pltpu.SemaphoreType.DMA((STORES + 2,))],
        compiler_params=pltpu.CompilerParams(vmem_limit_bytes=1024 * 1024),
        name="store_results",
    )(*results)


def solution(mesh):
    in_specs = (
        P("ep", None, "fs", None),
        P(),
        P("ep", "fs", None),
        P("ep", "fs", None),
        P("ep", "fs", None),
        P(),
        P(),
        P(),
        P(),
    )
    out_specs = (P("ep", None, None), P("ep", "fs", None), P("ep", "fs", None))
    body = functools.partial(per_device, mesh.shape["ep"])
    return jax.shard_map(
        body, mesh=mesh, in_specs=in_specs, out_specs=out_specs, check_vma=False
    )
```

```python
import functools

import jax
import jax.numpy as jnp
from jax import lax
from jax.experimental import pallas as pl
from jax.experimental.pallas import tpu as pltpu
from jax.sharding import PartitionSpec as P

MOMENTUM_DECAY = 0.9
SECOND_DECAY = 0.99
NORM_EPS = 1e-06
ROOT_EPS = 1e-08
STEP_SCALE = 0.2
EXP_SCALE = 0.5
LANES = 128
CORES = 2
SIDE = 4
CHUNKS = 16
PIECES = 8
LAG_ONE = 6
LAG_TWO = 11
LAG_THREE = 16
GATE_PIECE = 6
FIRST = 1
ORDER = (2, 1, 3, 0)
CODES = 32767.0
TINY = 1e-30
TILE = 896
STORES = 4
VMEM_BYTES = 67043328 - 9175040


def largest_divisor(number, most):
    return max(d for d in range(1, most + 1) if number % d == 0)


def tile_width(columns, most):
    return LANES * largest_divisor(columns // LANES, most // LANES)


def remote(src, dst, send_sem, recv_sem, axis, peer):
    return pltpu.make_async_remote_copy(
        src_ref=src,
        dst_ref=dst,
        send_sem=send_sem,
        recv_sem=recv_sem,
        device_id={axis: peer},
        device_id_type=pl.DeviceIdType.MESH,
    )


def kernel(
    ring,
    counts_hbm,
    in_weight_hbm,
    in_bias_hbm,
    out_weight_hbm,
    out_bias_hbm,
    grads_hbm,
    weight_hbm,
    mom_hbm,
    second_hbm,
    gathered_out,
    mom_out,
    second_out,
    counts,
    in_weight,
    in_bias,
    out_weight,
    out_bias,
    grads,
    weight,
    pair_out,
    pair_in,
    ring_out,
    ring_in,
    scale_out,
    scale_in,
    gradient,
    sums,
    layer,
    tally,
    small_sem,
    slab_sem,
    param_sem,
    pair_send,
    pair_recv,
    ring_send,
    ring_recv,
    scale_send,
    gate,
    ready,
    sum_send,
    sum_recv,
    row_send,
    pass_recv,
    last_recv,
):
    gathered = gathered_out.at[0]
    mom = mom_out.at[0]
    second = second_out.at[0]
    groups = ring * CORES
    shards = SIDE * SIDE
    rows, columns = gradient.shape
    units = in_bias.shape[0]
    me_group = lax.axis_index("ep")
    me = lax.axis_index("fs")
    y = me_group // CORES
    core = me_group % CORES
    partner = y * CORES + 1 - core
    z = me // SIDE
    x = me % SIDE

    def group_of(step, which):
        return (y + step) % ring * CORES + which

    small = [
        pltpu.make_async_copy(src, dst, small_sem.at[i])
        for i, (src, dst) in enumerate(
            (
                (counts_hbm, counts),
                (in_weight_hbm, in_weight),
                (in_bias_hbm, in_bias),
                (out_weight_hbm, out_weight),
                (out_bias_hbm, out_bias),
            )
        )
    ]
    for copy in small:
        copy.start()

    def slab(which, step):
        return pltpu.make_async_copy(
            grads_hbm.at[0, group_of(step, which)],
            grads.at[which, step],
            slab_sem.at[which],
        )

    def slabs_in(which):
        pltpu.make_async_copy(
            grads_hbm.at[0, pl.ds(0, ring)], grads.at[which], slab_sem.at[which]
        ).wait()

    for which in (FIRST, 1 - FIRST):
        for step in ORDER:
            slab(which, step).start()
    barrier = pltpu.get_barrier_semaphore()
    near = [
        {"fs": up * SIDE + along}
        for up, along in (
            (z, (x + 1) % SIDE),
            (z, (x + SIDE - 1) % SIDE),
            ((z + 1) % SIDE, x),
            ((z + SIDE - 1) % SIDE, x),
        )
    ]

    def greet(semaphore, peers):
        for peer in peers:
            pl.semaphore_signal(
                semaphore, inc=1, device_id=peer, device_id_type=pl.DeviceIdType.MESH
            )

    beside = [{"ep": peer} for peer in (partner, group_of(1, core), group_of(ring - 1, core))]
    greet(barrier, beside + near)
    small[0].wait()

    pieces = ring_recv.shape[1]
    piece = columns // pieces
    narrow = tile_width(piece, 512)

    def cols_of(p, i):
        return pl.ds(pl.multiple_of(p * piece + i * narrow, narrow), narrow)

    def piece_of(p):
        return pl.ds(pl.multiple_of(p * piece, piece), piece)

    def share_of(expert):
        total = counts[0, expert]
        for s in range(1, groups):
            total = total + counts[s, expert]
        mine = jnp.full((1, LANES), counts[me_group, expert].astype(jnp.float32))
        return (mine / jnp.full((1, LANES), total.astype(jnp.float32)))[:, :1]

    def weighted(share, which, step, cols):
        value = share * grads[which, step, :, cols].astype(jnp.float32)
        return value.astype(jnp.bfloat16)

    slabs_in(FIRST)
    pl.semaphore_wait(barrier, len(beside) + len(near))
    greet(ready.at[0], near)

    def pair_copy(part, p):
        slots = (pl.ds(0, 1), pl.ds(1, ring - 1))[part]
        return remote(
            pair_out.at[slots, :, piece_of(p)],
            pair_in.at[slots, :, piece_of(p)],
            pair_send.at[part],
            pair_recv.at[part, p],
            "ep",
            partner,
        )

    def give():
        shares = [share_of(group_of(step, 1 - core)) for step in range(ring)]
        for part, steps in enumerate((ORDER[:1], ORDER[1:])):

            def body(p, carry, part=part, steps=steps):
                for step in steps:
                    pair_out[ORDER.index(step), :, piece_of(p)] = weighted(
                        shares[step], 1 - core, step, piece_of(p)
                    )
                pair_copy(part, p).start()
                return carry

            lax.fori_loop(0, pieces, body, 0)

    def hop(slot, p, odd=0):
        step = (1 - 2 * odd, 1, -1)[slot]
        peer = group_of(step + ring, core)
        codes = remote(
            ring_out.at[slot, :, piece_of(p)],
            ring_in.at[slot, :, piece_of(p)],
            ring_send.at[slot],
            ring_recv.at[slot, p],
            "ep",
            peer,
        )
        scale = remote(
            scale_out.at[slot, p],
            scale_in.at[slot, p],
            scale_send.at[slot],
            ring_recv.at[slot, p],
            "ep",
            peer,
        )
        return codes, scale

    def landed(slot, p):
        remote(tally, tally, ring_send.at[slot], ring_recv.at[slot, p], "ep", partner).wait_recv()

    def spread_lanes(row, width):
        return jnp.concatenate([row] * (width // LANES), axis=1)

    def pair_sum(step, cols):
        total = weighted(shares[step], core, step, cols).astype(jnp.float32)
        return total + pair_in[ORDER.index(step), :, cols].astype(jnp.float32)

    def decode(slot, p, cols, width):
        codes = ring_in[slot, :, cols].astype(jnp.int32).astype(jnp.float32)
        return codes * spread_lanes(scale_in[slot, p], width)

    def encode(slot, p, odd, total):
        most = jnp.max(jnp.abs(total), axis=0, keepdims=True)
        parts = [most[:, j : j + LANES] for j in range(0, piece, LANES)]
        most = jnp.maximum(functools.reduce(jnp.maximum, parts), TINY)
        scale_out[slot, p] = most * (1.0 / CODES)
        codes = lax.round(
            total * spread_lanes(CODES / most, piece), lax.RoundingMethod.TO_NEAREST_EVEN
        )
        ring_out[slot, :, piece_of(p)] = codes.astype(jnp.int32).astype(jnp.int16)
        for copy in hop(slot, p, odd):
            copy.start()

    @pl.when(core != FIRST)
    def _():
        give()
        pl.semaphore_wait(gate, 1)

    shares = [share_of(group_of(step, core)) for step in range(ring)]
    @pl.when(core != FIRST)
    def _():
        slabs_in(1 - FIRST)

    def far(q, carry):
        for odd in range(2):
            p = 2 * q + odd
            pair_copy(0, p).wait_recv()
            encode(0, p, odd, pair_sum(2, piece_of(p)))
        return carry

    lax.fori_loop(0, pieces // 2, far, 0)

    def combine(q, carry):
        for odd in range(2):
            p = 2 * q + odd
            pair_copy(1, p).wait_recv()
            slot, step = ((2, 3), (1, 1))[odd]
            encode(slot, p, odd, pair_sum(step, piece_of(p)))
            slot, step = ((1, 1), (2, 3))[odd]
            landed(0, p)
            encode(slot, p, odd, pair_sum(step, piece_of(p)) + decode(0, p, piece_of(p), piece))
        return carry

    lax.fori_loop(0, pieces // 2, combine, 0)

    pl.semaphore_wait(ready.at[0], len(near))
    greet(ready.at[1], near)
    @pl.when(core == FIRST)
    def _():
        slabs_in(1 - FIRST)
        give()

    for copy in small[1:]:
        copy.wait()
    params = [
        pltpu.make_async_copy(src.at[0], dst, param_sem.at[i])
        for i, (src, dst) in enumerate(
            ((mom_hbm, mom), (second_hbm, second), (weight_hbm, weight))
        )
    ]
    for copy in params:
        copy.start()


    shape = (rows, layer.shape[1])
    lane = lax.broadcasted_iota(jnp.int32, shape, 1)
    slot = lane // rows
    diagonal = lane % rows == lax.broadcasted_iota(jnp.int32, shape, 0)

    def halves(value):
        high = value.astype(jnp.bfloat16).astype(jnp.float32)
        return high, value - high

    def place(h, carry):
        block = jnp.zeros(shape, jnp.float32)
        for f in range(5):
            high, low = halves(jnp.full(shape, in_weight[f, h]))
            whole = slot == f
            if f < 4:
                whole = jnp.logical_or(whole, slot == 5 + f)
            block = jnp.where(whole, high, jnp.where(slot == 9 + f, low, block))
        block = jnp.where(diagonal, block, 0.0)
        layer[pl.ds(pl.multiple_of(h * rows, rows), rows), :] = block.astype(jnp.bfloat16)
        return carry

    lax.fori_loop(0, units, place, 0)
    pl.semaphore_wait(ready.at[1], len(near))
    greet(ready.at[2], near)
    for copy in params:
        copy.wait()

    def moments(p, carry):
        for slot in (1, 2):
            landed(slot, p)

        @pl.when(jnp.logical_and(core == FIRST, p == GATE_PIECE))
        def _():
            pl.semaphore_signal(
                gate,
                inc=1,
                device_id={"ep": partner},
                device_id_type=pl.DeviceIdType.MESH,
            )

        def one(i, inner):
            grad_acc, mom_acc = inner
            cols = cols_of(p, i)
            total = pair_sum(0, cols) + decode(1, p, cols, narrow) + decode(2, p, cols, narrow)
            mom_next = MOMENTUM_DECAY * mom[:, cols] + (1.0 - MOMENTUM_DECAY) * total
            gradient[:, cols] = total
            mom[:, cols] = mom_next
            second[:, cols] = (
                SECOND_DECAY * second[:, cols] + (1.0 - SECOND_DECAY) * total * total
            )
            return grad_acc + total * total, mom_acc + mom_next * mom_next

        return lax.fori_loop(0, piece // narrow, one, carry, unroll=True)

    zero = jnp.zeros((rows, narrow), jnp.float32)
    grad_acc, mom_acc = lax.fori_loop(0, pieces, moments, (zero, zero))

    def to_lanes(acc):
        acc = jnp.sum(acc, axis=0, keepdims=True)
        return sum(acc[:, j : j + LANES] for j in range(0, narrow, LANES))

    pl.semaphore_wait(ready.at[2], len(near))
    sums[me, 0:1, :] = to_lanes(grad_acc)
    sums[me, 1:2, :] = to_lanes(mom_acc)
    for step in range(1, shards):
        remote(
            sums.at[me], sums.at[me], sum_send, sum_recv, "fs", (me + step) % shards
        ).start()
    others = sums.at[pl.ds(0, shards - 1)]
    all_sums = remote(others, others, sum_send, sum_recv, "fs", (me + 1) % shards)
    all_sums.wait_recv()

    entries = rows * columns * shards
    totals = sums[0]
    for s in range(1, shards):
        totals = totals + sums[s]
    mean = jnp.broadcast_to(jnp.sum(totals, axis=1, keepdims=True) / entries, (2, LANES)) + NORM_EPS
    inverse = lax.rsqrt(mean)
    inv_grad = inverse[0:1, :1]
    inv_mom = inverse[1:2, :1]
    log_mom = jnp.max(0.5 * jnp.log(mean[1:2, :]))
    tail = pl.ds(shape[1] - LANES, LANES)
    biased = slot[:, -LANES:] >= 14
    first = slot[:, -LANES:] == 14
    ends = diagonal[:, -LANES:]

    def settle(h, carry):
        high, low = halves(jnp.full(ends.shape, in_bias[h] + in_weight[5, h] * log_mom))
        span = pl.ds(pl.multiple_of(h * rows, rows), rows)
        block = jnp.where(ends, jnp.where(first, high, low), 0.0)
        kept = layer[span, tail].astype(jnp.float32)
        layer[span, tail] = jnp.where(biased, block, kept).astype(jnp.bfloat16)
        return carry

    lax.fori_loop(0, units, settle, 0)

    chunks = pass_recv.shape[1]
    width = columns // chunks
    tile = tile_width(width, TILE)

    def learned_step(cols):
        grad = gradient[:, cols]
        mom_next = mom[:, cols]
        narrow_old = weight[:, cols]
        inv_root = lax.rsqrt(second[:, cols] + ROOT_EPS)
        highs, lows = [], []
        for value in (
            grad * inv_grad,
            mom_next * inv_mom,
            mom_next * inv_root,
            grad * inv_root,
        ):
            high = value.astype(jnp.bfloat16)
            highs.append(high)
            lows.append((value - high.astype(jnp.float32)).astype(jnp.bfloat16))
        highs.append(narrow_old)
        ones = jnp.ones(grad.shape, jnp.bfloat16)
        features = jnp.concatenate(highs + lows + highs + [ones, ones], axis=0)
        hidden = jnp.dot(layer[...], features, preferred_element_type=jnp.float32)
        directions = [jnp.full(grad.shape, out_bias[0]), jnp.zeros(grad.shape, jnp.float32)]
        magnitudes = [jnp.full(grad.shape, out_bias[1]), jnp.zeros(grad.shape, jnp.float32)]
        for h in range(units):
            active = jnp.maximum(hidden[h * rows : (h + 1) * rows, :], 0.0)
            side = 2 * h // units
            directions[side] = directions[side] + active * out_weight[0, h]
            magnitudes[side] = magnitudes[side] + active * out_weight[1, h]
        direction = directions[0] + directions[1]
        magnitude = magnitudes[0] + magnitudes[1]
        update = STEP_SCALE * direction * jnp.exp(EXP_SCALE * magnitude)
        return (narrow_old.astype(jnp.float32) - update).astype(jnp.bfloat16)

    def rows_of(source):
        return pl.ds(pl.multiple_of(source * rows, rows), rows)

    def block(source, k):
        return gathered.at[rows_of(source), pl.ds(pl.multiple_of(k * width, width), width)]

    def route(k):
        swap = k % 2
        turn = 1 - 2 * (k // 2 % 2)

        def at(first, after):
            up = (z + 2 * SIDE + first * swap + after * (1 - swap)) % SIDE
            along = (x + 2 * SIDE + first * (1 - swap) + after * swap) % SIDE
            return up * SIDE + along

        return at, turn

    def send(source, k, role, recv, peer):
        remote(block(source, k), block(source, k), row_send.at[role], recv, "fs", peer).start()

    def spread(source, k, role, at, way):
        send(source, k, role, pass_recv.at[role, k], at(0, way))
        send(source, k, role, last_recv.at[source], at(0, -way))

    def arrive(stage, k, count):
        part = gathered.at[pl.ds(0, count * rows), pl.ds(pl.multiple_of(k * width, width), width)]
        remote(part, part, row_send.at[0], pass_recv.at[stage, k], "fs", me).wait_recv()

    def pass_on(k, role, first):
        at, turn = route(k)
        way = turn if first % 2 == 0 else -turn
        source = at(first * turn, -way)
        send(source, k, role, last_recv.at[source], at(0, way))

    def own(k):
        at, turn = route(k)
        send(me, k, 0, pass_recv.at[0, k], at(turn, 0))
        send(me, k, 0, pass_recv.at[0, k], at(-turn, 0))
        spread(me, k, 0, at, turn)

    def relay_one(k):
        at, turn = route(k)
        arrive(0, k, 3)
        source = at(-turn, 0)
        send(source, k, 1, pass_recv.at[1, k], at(turn, 0))
        spread(source, k, 1, at, -turn)
        spread(at(turn, 0), k, 1, at, -turn)
        pass_on(k, 1, 0)

    def relay_two(k):
        at, turn = route(k)
        arrive(1, k, 3)
        spread(at(2, 0), k, 2, at, turn)
        pass_on(k, 2, -1)
        pass_on(k, 2, 1)

    def relay_three(k):
        arrive(2, k, 1)
        pass_on(k, 3, 2)

    def turn_of(t, carry):
        for lag, relay in ((LAG_ONE, relay_one), (LAG_TWO, relay_two), (LAG_THREE, relay_three)):
            k = t - lag

            @pl.when(jnp.logical_and(k >= 0, k < chunks))
            def _(k=k, relay=relay):
                relay(k)

        @pl.when(t < chunks)
        def _():
            def one(i, inner):
                cols = pl.ds(pl.multiple_of(t * width + i * tile, tile), tile)
                gathered[rows_of(me), cols] = learned_step(cols)
                return inner

            lax.fori_loop(0, width // tile, one, 0)
            own(t)

        return carry

    lax.fori_loop(0, chunks + LAG_THREE, turn_of, 0)

    for part in range(2):
        slots = (pl.ds(0, 1), pl.ds(1, ring - 1))[part]
        remote(
            pair_out.at[slots], pair_in.at[slots], pair_send.at[part], pair_recv.at[part, 0], "ep", partner
        ).wait_send()
    for slot in range(3):
        remote(
            ring_out.at[slot], ring_in.at[slot], ring_send.at[slot], ring_recv.at[slot, 0], "ep", partner
        ).wait_send()
        remote(
            scale_out.at[slot], scale_in.at[slot], scale_send.at[slot], ring_recv.at[slot, 0], "ep", partner
        ).wait_send()
    all_sums.wait_send()
    share = {0: 0, 1: chunks // 4, 2: chunks // 2, 3: chunks // 4}
    for up in range(SIDE):
        for along in range(SIDE):
            number = share[up] + share[along]
            if number == 0:
                continue
            source = (z + up) % SIDE * SIDE + (x + along) % SIDE
            part = gathered.at[rows_of(source), pl.ds(0, number * width)]
            remote(part, part, row_send.at[0], last_recv.at[source], "fs", source).wait_recv()
    for role, number in enumerate((4, 6, 4, 1)):
        part = gathered.at[pl.ds(0, number * rows), :]
        remote(
            part, part, row_send.at[role], last_recv.at[me], "fs", (me + 1) % shards
        ).wait_send()


def store(gathered, mom, second, gathered_hbm, mom_hbm, second_hbm, sems):
    height = gathered.shape[1] // STORES
    copies = [
        pltpu.make_async_copy(
            gathered.at[:, pl.ds(i * height, height), :],
            gathered_hbm.at[:, pl.ds(i * height, height), :],
            sems.at[i],
        )
        for i in range(STORES)
    ]
    copies.append(pltpu.make_async_copy(mom, mom_hbm, sems.at[STORES]))
    copies.append(pltpu.make_async_copy(second, second_hbm, sems.at[STORES + 1]))
    for copy in copies:
        copy.start()
    for copy in copies:
        copy.wait()


def per_device(groups, grads, counts, weight, mom, second, in_weight, in_bias, out_weight, out_bias):
    rows, columns = mom.shape[1], mom.shape[2]
    ring = groups // CORES
    shards = SIDE * SIDE
    pieces = PIECES
    chunks = CHUNKS
    hbm = pl.BlockSpec(memory_space=pltpu.HBM)
    vmem = pl.BlockSpec(memory_space=pltpu.VMEM)
    results = pl.pallas_call(
        functools.partial(kernel, ring),
        out_shape=(
            pltpu.VMEM((1, rows * shards, columns), jnp.bfloat16),
            pltpu.VMEM(mom.shape, jnp.float32),
            pltpu.VMEM(second.shape, jnp.float32),
        ),
        in_specs=[hbm] * 9,
        out_specs=(vmem, vmem, vmem),
        scratch_shapes=[
            pltpu.SMEM(counts.shape, jnp.int32),
            pltpu.SMEM(in_weight.shape, jnp.float32),
            pltpu.SMEM(in_bias.shape, jnp.float32),
            pltpu.SMEM(out_weight.shape[::-1], jnp.float32),
            pltpu.SMEM(out_bias.shape, jnp.float32),
            pltpu.VMEM((CORES, ring, rows, columns), jnp.bfloat16),
            pltpu.VMEM((rows, columns), jnp.bfloat16),
            pltpu.VMEM((ring, rows, columns), jnp.bfloat16),
            pltpu.VMEM((ring, rows, columns), jnp.bfloat16),
            pltpu.VMEM((ring - 1, rows, columns), jnp.int16),
            pltpu.VMEM((ring - 1, rows, columns), jnp.int16),
            pltpu.VMEM((ring - 1, pieces, 1, LANES), jnp.float32),
            pltpu.VMEM((ring - 1, pieces, 1, LANES), jnp.float32),
            pltpu.VMEM((rows, columns), jnp.float32),
            pltpu.VMEM((shards, 2, LANES), jnp.float32),
            pltpu.VMEM((in_bias.shape[0] * rows, 16 * rows), jnp.bfloat16),
            pltpu.VMEM((rows * columns // pieces * 2 // (4 * LANES) + 1, LANES), jnp.float32),
            pltpu.SemaphoreType.DMA((5,)),
            pltpu.SemaphoreType.DMA((CORES,)),
            pltpu.SemaphoreType.DMA((3,)),
            pltpu.SemaphoreType.DMA((2,)),
            pltpu.SemaphoreType.DMA((2, pieces)),
            pltpu.SemaphoreType.DMA((ring - 1,)),
            pltpu.SemaphoreType.DMA((ring - 1, pieces)),
            pltpu.SemaphoreType.DMA((ring - 1,)),
            pltpu.SemaphoreType.REGULAR,
            pltpu.SemaphoreType.REGULAR((3,)),
            pltpu.SemaphoreType.DMA,
            pltpu.SemaphoreType.DMA,
            pltpu.SemaphoreType.DMA((4,)),
            pltpu.SemaphoreType.DMA((3, chunks)),
            pltpu.SemaphoreType.DMA((shards,)),
        ],
        compiler_params=pltpu.CompilerParams(
            collective_id=0, has_side_effects=True, vmem_limit_bytes=VMEM_BYTES
        ),
        name="learned_update",
    )(counts, in_weight, in_bias, out_weight.T, out_bias, grads, weight, mom, second)
    return pl.pallas_call(
        store,
        out_shape=[jax.ShapeDtypeStruct(r.shape, r.dtype) for r in results],
        in_specs=[vmem] * 3,
        out_specs=[hbm] * 3,
        scratch_shapes=[pltpu.SemaphoreType.DMA((STORES + 2,))],
        compiler_params=pltpu.CompilerParams(vmem_limit_bytes=1024 * 1024),
        name="store_results",
    )(*results)


def solution(mesh):
    in_specs = (
        P("ep", None, "fs", None),
        P(),
        P("ep", "fs", None),
        P("ep", "fs", None),
        P("ep", "fs", None),
        P(),
        P(),
        P(),
        P(),
    )
    out_specs = (P("ep", None, None), P("ep", "fs", None), P("ep", "fs", None))
    body = functools.partial(per_device, mesh.shape["ep"])
    return jax.shard_map(
        body, mesh=mesh, in_specs=in_specs, out_specs=out_specs, check_vma=False
    )
```

```python
import functools

import jax
import jax.numpy as jnp
from jax import lax
from jax.experimental import pallas as pl
from jax.experimental.pallas import tpu as pltpu
from jax.sharding import PartitionSpec as P

MOMENTUM_DECAY = 0.9
SECOND_DECAY = 0.99
NORM_EPS = 1e-06
ROOT_EPS = 1e-08
STEP_SCALE = 0.2
EXP_SCALE = 0.5
LANES = 128
CORES = 2
SIDE = 4
CHUNKS = 16
PIECES = 8
LAG_ONE = 6
LAG_TWO = 11
LAG_THREE = 16
GATE_PIECE = 6
FIRST = 1
ORDER = (2, 1, 3, 0)
CODES = 32767.0
TINY = 1e-30
TILE = 896
STORES = 4
VMEM_BYTES = 67043328 - 9175040


def largest_divisor(number, most):
    return max(d for d in range(1, most + 1) if number % d == 0)


def tile_width(columns, most):
    return LANES * largest_divisor(columns // LANES, most // LANES)


def remote(src, dst, send_sem, recv_sem, axis, peer):
    return pltpu.make_async_remote_copy(
        src_ref=src,
        dst_ref=dst,
        send_sem=send_sem,
        recv_sem=recv_sem,
        device_id={axis: peer},
        device_id_type=pl.DeviceIdType.MESH,
    )


def kernel(
    ring,
    counts_hbm,
    in_weight_hbm,
    in_bias_hbm,
    out_weight_hbm,
    out_bias_hbm,
    grads_hbm,
    weight_hbm,
    mom_hbm,
    second_hbm,
    gathered_out,
    mom_out,
    second_out,
    counts,
    in_weight,
    in_bias,
    out_weight,
    out_bias,
    grads,
    weight,
    pair_out,
    pair_in,
    ring_out,
    ring_in,
    scale_out,
    scale_in,
    gradient,
    sums,
    layer,
    tally,
    small_sem,
    slab_sem,
    param_sem,
    pair_send,
    pair_recv,
    ring_send,
    ring_recv,
    scale_send,
    gate,
    ready,
    sum_send,
    sum_recv,
    row_send,
    pass_recv,
    last_recv,
):
    gathered = gathered_out.at[0]
    mom = mom_out.at[0]
    second = second_out.at[0]
    groups = ring * CORES
    shards = SIDE * SIDE
    rows, columns = gradient.shape
    units = in_bias.shape[0]
    me_group = lax.axis_index("ep")
    me = lax.axis_index("fs")
    y = me_group // CORES
    core = me_group % CORES
    partner = y * CORES + 1 - core
    z = me // SIDE
    x = me % SIDE

    def group_of(step, which):
        return (y + step) % ring * CORES + which

    small = [
        pltpu.make_async_copy(src, dst, small_sem.at[i])
        for i, (src, dst) in enumerate(
            (
                (counts_hbm, counts),
                (in_weight_hbm, in_weight),
                (in_bias_hbm, in_bias),
                (out_weight_hbm, out_weight),
                (out_bias_hbm, out_bias),
            )
        )
    ]
    for copy in small:
        copy.start()

    def slab(which, step):
        return pltpu.make_async_copy(
            grads_hbm.at[0, group_of(step, which)],
            grads.at[which, step],
            slab_sem.at[which],
        )

    def slabs_in(which):
        pltpu.make_async_copy(
            grads_hbm.at[0, pl.ds(0, ring)], grads.at[which], slab_sem.at[which]
        ).wait()

    for which in (FIRST, 1 - FIRST):
        for step in ORDER:
            slab(which, step).start()
    barrier = pltpu.get_barrier_semaphore()
    near = [
        {"fs": up * SIDE + along}
        for up, along in (
            (z, (x + 1) % SIDE),
            (z, (x + SIDE - 1) % SIDE),
            ((z + 1) % SIDE, x),
            ((z + SIDE - 1) % SIDE, x),
        )
    ]

    def greet(semaphore, peers):
        for peer in peers:
            pl.semaphore_signal(
                semaphore, inc=1, device_id=peer, device_id_type=pl.DeviceIdType.MESH
            )

    beside = [{"ep": peer} for peer in (partner, group_of(1, core), group_of(ring - 1, core))]
    greet(barrier, beside + near)
    small[0].wait()

    pieces = ring_recv.shape[1]
    piece = columns // pieces
    narrow = tile_width(piece, 512)

    def cols_of(p, i):
        return pl.ds(pl.multiple_of(p * piece + i * narrow, narrow), narrow)

    def piece_of(p):
        return pl.ds(pl.multiple_of(p * piece, piece), piece)

    def share_of(expert):
        total = counts[0, expert]
        for s in range(1, groups):
            total = total + counts[s, expert]
        mine = jnp.full((1, LANES), counts[me_group, expert].astype(jnp.float32))
        return (mine / jnp.full((1, LANES), total.astype(jnp.float32)))[:, :1]

    def weighted(share, which, step, cols):
        value = share * grads[which, step, :, cols].astype(jnp.float32)
        return value.astype(jnp.bfloat16)

    slabs_in(FIRST)
    pl.semaphore_wait(barrier, len(beside) + len(near))
    greet(ready.at[0], near)

    def pair_copy(part, p):
        slots = (pl.ds(0, 1), pl.ds(1, ring - 1))[part]
        return remote(
            pair_out.at[slots, :, piece_of(p)],
            pair_in.at[slots, :, piece_of(p)],
            pair_send.at[part],
            pair_recv.at[part, p],
            "ep",
            partner,
        )

    def give():
        shares = [share_of(group_of(step, 1 - core)) for step in range(ring)]
        for part, steps in enumerate((ORDER[:1], ORDER[1:])):

            def body(p, carry, part=part, steps=steps):
                for step in steps:
                    pair_out[ORDER.index(step), :, piece_of(p)] = weighted(
                        shares[step], 1 - core, step, piece_of(p)
                    )
                pair_copy(part, p).start()
                return carry

            lax.fori_loop(0, pieces, body, 0)

    def hop(slot, p, odd=0):
        step = (1 - 2 * odd, 1, -1)[slot]
        peer = group_of(step + ring, core)
        codes = remote(
            ring_out.at[slot, :, piece_of(p)],
            ring_in.at[slot, :, piece_of(p)],
            ring_send.at[slot],
            ring_recv.at[slot, p],
            "ep",
            peer,
        )
        scale = remote(
            scale_out.at[slot, p],
            scale_in.at[slot, p],
            scale_send.at[slot],
            ring_recv.at[slot, p],
            "ep",
            peer,
        )
        return codes, scale

    def landed(slot, p):
        remote(tally, tally, ring_send.at[slot], ring_recv.at[slot, p], "ep", partner).wait_recv()

    def spread_lanes(row, width):
        return jnp.concatenate([row] * (width // LANES), axis=1)

    def pair_sum(step, cols):
        total = weighted(shares[step], core, step, cols).astype(jnp.float32)
        return total + pair_in[ORDER.index(step), :, cols].astype(jnp.float32)

    def decode(slot, p, cols, width):
        codes = ring_in[slot, :, cols].astype(jnp.int32).astype(jnp.float32)
        return codes * spread_lanes(scale_in[slot, p], width)

    def encode(slot, p, odd, total):
        most = jnp.max(jnp.abs(total), axis=0, keepdims=True)
        parts = [most[:, j : j + LANES] for j in range(0, piece, LANES)]
        most = jnp.maximum(functools.reduce(jnp.maximum, parts), TINY)
        scale_out[slot, p] = most * (1.0 / CODES)
        codes = lax.round(
            total * spread_lanes(CODES / most, piece), lax.RoundingMethod.TO_NEAREST_EVEN
        )
        ring_out[slot, :, piece_of(p)] = codes.astype(jnp.int32).astype(jnp.int16)
        for copy in hop(slot, p, odd):
            copy.start()

    @pl.when(core != FIRST)
    def _():
        give()
        pl.semaphore_wait(gate, 1)

    shares = [share_of(group_of(step, core)) for step in range(ring)]
    @pl.when(core != FIRST)
    def _():
        slabs_in(1 - FIRST)

    def far(q, carry):
        for odd in range(2):
            p = 2 * q + odd
            pair_copy(0, p).wait_recv()
            encode(0, p, odd, pair_sum(2, piece_of(p)))
        return carry

    lax.fori_loop(0, pieces // 2, far, 0)

    def combine(q, carry):
        for odd in range(2):
            p = 2 * q + odd
            pair_copy(1, p).wait_recv()
            slot, step = ((2, 3), (1, 1))[odd]
            encode(slot, p, odd, pair_sum(step, piece_of(p)))
            slot, step = ((1, 1), (2, 3))[odd]
            landed(0, p)
            encode(slot, p, odd, pair_sum(step, piece_of(p)) + decode(0, p, piece_of(p), piece))
        return carry

    lax.fori_loop(0, pieces // 2, combine, 0)

    pl.semaphore_wait(ready.at[0], len(near))
    greet(ready.at[1], near)
    @pl.when(core == FIRST)
    def _():
        slabs_in(1 - FIRST)
        give()

    for copy in small[1:]:
        copy.wait()
    params = [
        pltpu.make_async_copy(src.at[0], dst, param_sem.at[i])
        for i, (src, dst) in enumerate(
            ((mom_hbm, mom), (second_hbm, second), (weight_hbm, weight))
        )
    ]
    for copy in params:
        copy.start()


    shape = (rows, layer.shape[1])
    lane = lax.broadcasted_iota(jnp.int32, shape, 1)
    slot = lane // rows
    diagonal = lane % rows == lax.broadcasted_iota(jnp.int32, shape, 0)

    def halves(value):
        high = value.astype(jnp.bfloat16).astype(jnp.float32)
        return high, value - high

    def place(h, carry):
        block = jnp.zeros(shape, jnp.float32)
        for f in range(5):
            high, low = halves(jnp.full(shape, in_weight[f, h]))
            whole = slot == f
            if f < 4:
                whole = jnp.logical_or(whole, slot == 5 + f)
            block = jnp.where(whole, high, jnp.where(slot == 9 + f, low, block))
        block = jnp.where(diagonal, block, 0.0)
        layer[pl.ds(pl.multiple_of(h * rows, rows), rows), :] = block.astype(jnp.bfloat16)
        return carry

    lax.fori_loop(0, units, place, 0)
    pl.semaphore_wait(ready.at[1], len(near))
    greet(ready.at[2], near)
    for copy in params:
        copy.wait()

    def moments(p, carry):
        for slot in (1, 2):
            landed(slot, p)

        @pl.when(jnp.logical_and(core == FIRST, p == GATE_PIECE))
        def _():
            pl.semaphore_signal(
                gate,
                inc=1,
                device_id={"ep": partner},
                device_id_type=pl.DeviceIdType.MESH,
            )

        def one(i, inner):
            grad_acc, mom_acc = inner
            cols = cols_of(p, i)
            total = pair_sum(0, cols) + decode(1, p, cols, narrow) + decode(2, p, cols, narrow)
            mom_next = MOMENTUM_DECAY * mom[:, cols] + (1.0 - MOMENTUM_DECAY) * total
            gradient[:, cols] = total
            mom[:, cols] = mom_next
            second[:, cols] = (
                SECOND_DECAY * second[:, cols] + (1.0 - SECOND_DECAY) * total * total
            )
            return grad_acc + total * total, mom_acc + mom_next * mom_next

        return lax.fori_loop(0, piece // narrow, one, carry, unroll=True)

    zero = jnp.zeros((rows, narrow), jnp.float32)
    grad_acc, mom_acc = lax.fori_loop(0, pieces, moments, (zero, zero))

    def to_lanes(acc):
        acc = jnp.sum(acc, axis=0, keepdims=True)
        return sum(acc[:, j : j + LANES] for j in range(0, narrow, LANES))

    pl.semaphore_wait(ready.at[2], len(near))
    sums[me, 0:1, :] = to_lanes(grad_acc)
    sums[me, 1:2, :] = to_lanes(mom_acc)
    for step in range(1, shards):
        remote(
            sums.at[me], sums.at[me], sum_send, sum_recv, "fs", (me + step) % shards
        ).start()
    others = sums.at[pl.ds(0, shards - 1)]
    all_sums = remote(others, others, sum_send, sum_recv, "fs", (me + 1) % shards)
    all_sums.wait_recv()

    entries = rows * columns * shards
    totals = sums[0]
    for s in range(1, shards):
        totals = totals + sums[s]
    mean = jnp.broadcast_to(jnp.sum(totals, axis=1, keepdims=True) / entries, (2, LANES)) + NORM_EPS
    inverse = lax.rsqrt(mean)
    log_mom = 0.5 * jnp.log(mean[1:2, :])
    tail = pl.ds(shape[1] - LANES, LANES)
    biased = slot[:, -LANES:] >= 14
    first = slot[:, -LANES:] == 14
    ends = diagonal[:, -LANES:]

    def settle(h, carry):
        value = in_bias[h] + in_weight[5, h] * log_mom
        high, low = halves(jnp.broadcast_to(value, ends.shape))
        span = pl.ds(pl.multiple_of(h * rows, rows), rows)
        block = jnp.where(ends, jnp.where(first, high, low), 0.0)
        kept = layer[span, tail].astype(jnp.float32)
        layer[span, tail] = jnp.where(biased, block, kept).astype(jnp.bfloat16)
        return carry

    lax.fori_loop(0, units, settle, 0, unroll=True)

    chunks = pass_recv.shape[1]
    width = columns // chunks
    tile = tile_width(width, TILE)
    inv_grad = spread_lanes(inverse[0:1, :], tile)
    inv_mom = spread_lanes(inverse[1:2, :], tile)

    def learned_step(cols):
        grad = gradient[:, cols]
        mom_next = mom[:, cols]
        narrow_old = weight[:, cols]
        inv_root = lax.rsqrt(second[:, cols] + ROOT_EPS)
        highs, lows = [], []
        for value in (
            grad * inv_grad,
            mom_next * inv_mom,
            mom_next * inv_root,
            grad * inv_root,
        ):
            high = value.astype(jnp.bfloat16)
            highs.append(high)
            lows.append((value - high.astype(jnp.float32)).astype(jnp.bfloat16))
        highs.append(narrow_old)
        ones = jnp.ones(grad.shape, jnp.bfloat16)
        features = jnp.concatenate(highs + lows + highs + [ones, ones], axis=0)
        hidden = jnp.dot(layer[...], features, preferred_element_type=jnp.float32)
        directions = [jnp.full(grad.shape, out_bias[0]), jnp.zeros(grad.shape, jnp.float32)]
        magnitudes = [jnp.full(grad.shape, out_bias[1]), jnp.zeros(grad.shape, jnp.float32)]
        for h in range(units):
            active = jnp.maximum(hidden[h * rows : (h + 1) * rows, :], 0.0)
            side = 2 * h // units
            directions[side] = directions[side] + active * out_weight[0, h]
            magnitudes[side] = magnitudes[side] + active * out_weight[1, h]
        direction = directions[0] + directions[1]
        magnitude = magnitudes[0] + magnitudes[1]
        update = STEP_SCALE * direction * jnp.exp(EXP_SCALE * magnitude)
        return (narrow_old.astype(jnp.float32) - update).astype(jnp.bfloat16)

    def rows_of(source):
        return pl.ds(pl.multiple_of(source * rows, rows), rows)

    def block(source, k):
        return gathered.at[rows_of(source), pl.ds(pl.multiple_of(k * width, width), width)]

    def route(k):
        swap = k % 2
        turn = 1 - 2 * (k // 2 % 2)

        def at(first, after):
            up = (z + 2 * SIDE + first * swap + after * (1 - swap)) % SIDE
            along = (x + 2 * SIDE + first * (1 - swap) + after * swap) % SIDE
            return up * SIDE + along

        return at, turn

    def send(source, k, role, recv, peer):
        remote(block(source, k), block(source, k), row_send.at[role], recv, "fs", peer).start()

    def spread(source, k, role, at, way):
        send(source, k, role, pass_recv.at[role, k], at(0, way))
        send(source, k, role, last_recv, at(0, -way))

    def arrive(stage, k, count):
        part = gathered.at[pl.ds(0, count * rows), pl.ds(pl.multiple_of(k * width, width), width)]
        remote(part, part, row_send.at[0], pass_recv.at[stage, k], "fs", me).wait_recv()

    def pass_on(k, role, first):
        at, turn = route(k)
        way = turn if first % 2 == 0 else -turn
        source = at(first * turn, -way)
        send(source, k, role, last_recv, at(0, way))

    def own(k):
        at, turn = route(k)
        send(me, k, 0, pass_recv.at[0, k], at(turn, 0))
        send(me, k, 0, pass_recv.at[0, k], at(-turn, 0))
        spread(me, k, 0, at, turn)

    def relay_one(k):
        at, turn = route(k)
        arrive(0, k, 3)
        source = at(-turn, 0)
        send(source, k, 1, pass_recv.at[1, k], at(turn, 0))
        spread(source, k, 1, at, -turn)
        spread(at(turn, 0), k, 1, at, -turn)
        pass_on(k, 1, 0)

    def relay_two(k):
        at, turn = route(k)
        arrive(1, k, 3)
        spread(at(2, 0), k, 2, at, turn)
        pass_on(k, 2, -1)
        pass_on(k, 2, 1)

    def relay_three(k):
        arrive(2, k, 1)
        pass_on(k, 3, 2)

    def turn_of(t, carry):
        for lag, relay in ((LAG_ONE, relay_one), (LAG_TWO, relay_two), (LAG_THREE, relay_three)):
            k = t - lag

            @pl.when(jnp.logical_and(k >= 0, k < chunks))
            def _(k=k, relay=relay):
                relay(k)

        @pl.when(t < chunks)
        def _():
            def one(i, inner):
                cols = pl.ds(pl.multiple_of(t * width + i * tile, tile), tile)
                gathered[rows_of(me), cols] = learned_step(cols)
                return inner

            lax.fori_loop(0, width // tile, one, 0)
            own(t)

        return carry

    lax.fori_loop(0, chunks + LAG_THREE, turn_of, 0)

    for part in range(2):
        slots = (pl.ds(0, 1), pl.ds(1, ring - 1))[part]
        remote(
            pair_out.at[slots], pair_in.at[slots], pair_send.at[part], pair_recv.at[part, 0], "ep", partner
        ).wait_send()
    for slot in range(3):
        remote(
            ring_out.at[slot], ring_in.at[slot], ring_send.at[slot], ring_recv.at[slot, 0], "ep", partner
        ).wait_send()
        remote(
            scale_out.at[slot], scale_in.at[slot], scale_send.at[slot], ring_recv.at[slot, 0], "ep", partner
        ).wait_send()
    all_sums.wait_send()
    part = gathered.at[pl.ds(0, 8 * rows), :]
    remote(part, part, row_send.at[0], last_recv, "fs", me).wait_recv()
    for role, number in enumerate((4, 6, 4, 1)):
        part = gathered.at[pl.ds(0, number * rows), :]
        remote(
            part, part, row_send.at[role], last_recv, "fs", (me + 1) % shards
        ).wait_send()


def store(gathered, mom, second, gathered_hbm, mom_hbm, second_hbm, sems):
    height = gathered.shape[1] // STORES
    copies = [
        pltpu.make_async_copy(
            gathered.at[:, pl.ds(i * height, height), :],
            gathered_hbm.at[:, pl.ds(i * height, height), :],
            sems.at[i],
        )
        for i in range(STORES)
    ]
    copies.append(pltpu.make_async_copy(mom, mom_hbm, sems.at[STORES]))
    copies.append(pltpu.make_async_copy(second, second_hbm, sems.at[STORES + 1]))
    for copy in copies:
        copy.start()
    for copy in copies:
        copy.wait()


def per_device(groups, grads, counts, weight, mom, second, in_weight, in_bias, out_weight, out_bias):
    rows, columns = mom.shape[1], mom.shape[2]
    ring = groups // CORES
    shards = SIDE * SIDE
    pieces = PIECES
    chunks = CHUNKS
    hbm = pl.BlockSpec(memory_space=pltpu.HBM)
    vmem = pl.BlockSpec(memory_space=pltpu.VMEM)
    results = pl.pallas_call(
        functools.partial(kernel, ring),
        out_shape=(
            pltpu.VMEM((1, rows * shards, columns), jnp.bfloat16),
            pltpu.VMEM(mom.shape, jnp.float32),
            pltpu.VMEM(second.shape, jnp.float32),
        ),
        in_specs=[hbm] * 9,
        out_specs=(vmem, vmem, vmem),
        scratch_shapes=[
            pltpu.SMEM(counts.shape, jnp.int32),
            pltpu.SMEM(in_weight.shape, jnp.float32),
            pltpu.SMEM(in_bias.shape, jnp.float32),
            pltpu.SMEM(out_weight.shape[::-1], jnp.float32),
            pltpu.SMEM(out_bias.shape, jnp.float32),
            pltpu.VMEM((CORES, ring, rows, columns), jnp.bfloat16),
            pltpu.VMEM((rows, columns), jnp.bfloat16),
            pltpu.VMEM((ring, rows, columns), jnp.bfloat16),
            pltpu.VMEM((ring, rows, columns), jnp.bfloat16),
            pltpu.VMEM((ring - 1, rows, columns), jnp.int16),
            pltpu.VMEM((ring - 1, rows, columns), jnp.int16),
            pltpu.VMEM((ring - 1, pieces, 1, LANES), jnp.float32),
            pltpu.VMEM((ring - 1, pieces, 1, LANES), jnp.float32),
            pltpu.VMEM((rows, columns), jnp.float32),
            pltpu.VMEM((shards, 2, LANES), jnp.float32),
            pltpu.VMEM((in_bias.shape[0] * rows, 16 * rows), jnp.bfloat16),
            pltpu.VMEM((rows * columns // pieces * 2 // (4 * LANES) + 1, LANES), jnp.float32),
            pltpu.SemaphoreType.DMA((5,)),
            pltpu.SemaphoreType.DMA((CORES,)),
            pltpu.SemaphoreType.DMA((3,)),
            pltpu.SemaphoreType.DMA((2,)),
            pltpu.SemaphoreType.DMA((2, pieces)),
            pltpu.SemaphoreType.DMA((ring - 1,)),
            pltpu.SemaphoreType.DMA((ring - 1, pieces)),
            pltpu.SemaphoreType.DMA((ring - 1,)),
            pltpu.SemaphoreType.REGULAR,
            pltpu.SemaphoreType.REGULAR((3,)),
            pltpu.SemaphoreType.DMA,
            pltpu.SemaphoreType.DMA,
            pltpu.SemaphoreType.DMA((4,)),
            pltpu.SemaphoreType.DMA((3, chunks)),
            pltpu.SemaphoreType.DMA,
        ],
        compiler_params=pltpu.CompilerParams(
            collective_id=0, has_side_effects=True, vmem_limit_bytes=VMEM_BYTES
        ),
        name="learned_update",
    )(counts, in_weight, in_bias, out_weight.T, out_bias, grads, weight, mom, second)
    return pl.pallas_call(
        store,
        out_shape=[jax.ShapeDtypeStruct(r.shape, r.dtype) for r in results],
        in_specs=[vmem] * 3,
        out_specs=[hbm] * 3,
        scratch_shapes=[pltpu.SemaphoreType.DMA((STORES + 2,))],
        compiler_params=pltpu.CompilerParams(vmem_limit_bytes=1024 * 1024),
        name="store_results",
    )(*results)


def solution(mesh):
    in_specs = (
        P("ep", None, "fs", None),
        P(),
        P("ep", "fs", None),
        P("ep", "fs", None),
        P("ep", "fs", None),
        P(),
        P(),
        P(),
        P(),
    )
    out_specs = (P("ep", None, None), P("ep", "fs", None), P("ep", "fs", None))
    body = functools.partial(per_device, mesh.shape["ep"])
    return jax.shard_map(
        body, mesh=mesh, in_specs=in_specs, out_specs=out_specs, check_vma=False
    )
```

```python
import functools

import jax
import jax.numpy as jnp
from jax import lax
from jax.experimental import pallas as pl
from jax.experimental.pallas import tpu as pltpu
from jax.sharding import PartitionSpec as P

MOMENTUM_DECAY = 0.9
SECOND_DECAY = 0.99
NORM_EPS = 1e-06
ROOT_EPS = 1e-08
STEP_SCALE = 0.2
EXP_SCALE = 0.5
LANES = 128
CORES = 2
SIDE = 4
CHUNKS = 16
PIECES = 8
LAG_ONE = 6
LAG_TWO = 11
LAG_THREE = 16
GATE_PIECE = 6
FIRST = 1
ORDER = (2, 1, 3, 0)
CODES = 32767.0
TINY = 1e-30
TILE = 896
STORES = 4
VMEM_BYTES = 67043328 - 9175040


def largest_divisor(number, most):
    return max(d for d in range(1, most + 1) if number % d == 0)


def tile_width(columns, most):
    return LANES * largest_divisor(columns // LANES, most // LANES)


def remote(src, dst, send_sem, recv_sem, axis, peer):
    return pltpu.make_async_remote_copy(
        src_ref=src,
        dst_ref=dst,
        send_sem=send_sem,
        recv_sem=recv_sem,
        device_id={axis: peer},
        device_id_type=pl.DeviceIdType.MESH,
    )


def kernel(
    ring,
    counts_hbm,
    in_weight_hbm,
    in_bias_hbm,
    out_weight_hbm,
    out_bias_hbm,
    grads_hbm,
    weight_hbm,
    mom_hbm,
    second_hbm,
    gathered_out,
    mom_out,
    second_out,
    counts,
    in_weight,
    in_bias,
    out_weight,
    out_bias,
    grads,
    weight,
    pair_out,
    pair_in,
    ring_out,
    ring_in,
    scale_out,
    scale_in,
    gradient,
    sums,
    layer,
    tally,
    small_sem,
    slab_sem,
    param_sem,
    pair_send,
    pair_recv,
    ring_send,
    ring_recv,
    scale_send,
    gate,
    ready,
    sum_send,
    sum_recv,
    row_send,
    pass_recv,
    last_recv,
):
    gathered = gathered_out.at[0]
    mom = mom_out.at[0]
    second = second_out.at[0]
    groups = ring * CORES
    shards = SIDE * SIDE
    rows, columns = gradient.shape
    units = in_bias.shape[0]
    me_group = lax.axis_index("ep")
    me = lax.axis_index("fs")
    y = me_group // CORES
    core = me_group % CORES
    partner = y * CORES + 1 - core
    z = me // SIDE
    x = me % SIDE

    def group_of(step, which):
        return (y + step) % ring * CORES + which

    small = [
        pltpu.make_async_copy(src, dst, small_sem.at[i])
        for i, (src, dst) in enumerate(
            (
                (counts_hbm, counts),
                (in_weight_hbm, in_weight),
                (in_bias_hbm, in_bias),
                (out_weight_hbm, out_weight),
                (out_bias_hbm, out_bias),
            )
        )
    ]
    for copy in small:
        copy.start()

    def slab(which, step):
        return pltpu.make_async_copy(
            grads_hbm.at[0, group_of(step, which)],
            grads.at[which, step],
            slab_sem.at[which],
        )

    def slabs_in(which):
        pltpu.make_async_copy(
            grads_hbm.at[0, pl.ds(0, ring)], grads.at[which], slab_sem.at[which]
        ).wait()

    for which in (FIRST, 1 - FIRST):
        for step in ORDER:
            slab(which, step).start()
    barrier = pltpu.get_barrier_semaphore()
    near = [
        {"fs": up * SIDE + along}
        for up, along in (
            (z, (x + 1) % SIDE),
            (z, (x + SIDE - 1) % SIDE),
            ((z + 1) % SIDE, x),
            ((z + SIDE - 1) % SIDE, x),
        )
    ]

    def greet(semaphore, peers):
        for peer in peers:
            pl.semaphore_signal(
                semaphore, inc=1, device_id=peer, device_id_type=pl.DeviceIdType.MESH
            )

    beside = [{"ep": peer} for peer in (partner, group_of(1, core), group_of(ring - 1, core))]
    greet(barrier, beside + near)
    small[0].wait()

    pieces = ring_recv.shape[1]
    piece = columns // pieces
    narrow = tile_width(piece, 512)

    def cols_of(p, i):
        return pl.ds(pl.multiple_of(p * piece + i * narrow, narrow), narrow)

    def piece_of(p):
        return pl.ds(pl.multiple_of(p * piece, piece), piece)

    def share_of(expert):
        total = counts[0, expert]
        for s in range(1, groups):
            total = total + counts[s, expert]
        mine = jnp.full((1, LANES), counts[me_group, expert].astype(jnp.float32))
        return (mine / jnp.full((1, LANES), total.astype(jnp.float32)))[:, :1]

    def weighted(share, which, step, cols):
        value = share * grads[which, step, :, cols].astype(jnp.float32)
        return value.astype(jnp.bfloat16)

    slabs_in(FIRST)
    pl.semaphore_wait(barrier, len(beside) + len(near))
    greet(ready.at[0], near)

    def pair_copy(part, p):
        slots = (pl.ds(0, 1), pl.ds(1, ring - 1))[part]
        return remote(
            pair_out.at[slots, :, piece_of(p)],
            pair_in.at[slots, :, piece_of(p)],
            pair_send.at[part],
            pair_recv.at[part, p],
            "ep",
            partner,
        )

    def give():
        shares = [share_of(group_of(step, 1 - core)) for step in range(ring)]
        for part, steps in enumerate((ORDER[:1], ORDER[1:])):

            def body(p, carry, part=part, steps=steps):
                for step in steps:
                    pair_out[ORDER.index(step), :, piece_of(p)] = weighted(
                        shares[step], 1 - core, step, piece_of(p)
                    )
                pair_copy(part, p).start()
                return carry

            lax.fori_loop(0, pieces, body, 0)

    def hop(slot, p, odd=0):
        step = (1 - 2 * odd, 1, -1)[slot]
        peer = group_of(step + ring, core)
        codes = remote(
            ring_out.at[slot, :, piece_of(p)],
            ring_in.at[slot, :, piece_of(p)],
            ring_send.at[slot],
            ring_recv.at[slot, p],
            "ep",
            peer,
        )
        scale = remote(
            scale_out.at[slot, p],
            scale_in.at[slot, p],
            scale_send.at[slot],
            ring_recv.at[slot, p],
            "ep",
            peer,
        )
        return codes, scale

    def landed(slot, p):
        remote(tally, tally, ring_send.at[slot], ring_recv.at[slot, p], "ep", partner).wait_recv()

    def spread_lanes(row, width):
        return jnp.concatenate([row] * (width // LANES), axis=1)

    def pair_sum(step, cols):
        total = weighted(shares[step], core, step, cols).astype(jnp.float32)
        return total + pair_in[ORDER.index(step), :, cols].astype(jnp.float32)

    def decode(slot, p, cols, width):
        codes = ring_in[slot, :, cols].astype(jnp.int32).astype(jnp.float32)
        return codes * spread_lanes(scale_in[slot, p], width)

    def encode(slot, p, odd, total):
        most = jnp.max(jnp.abs(total), axis=0, keepdims=True)
        parts = [most[:, j : j + LANES] for j in range(0, piece, LANES)]
        most = jnp.maximum(functools.reduce(jnp.maximum, parts), TINY)
        scale_out[slot, p] = most * (1.0 / CODES)
        codes = lax.round(
            total * spread_lanes(CODES / most, piece), lax.RoundingMethod.TO_NEAREST_EVEN
        )
        ring_out[slot, :, piece_of(p)] = codes.astype(jnp.int32).astype(jnp.int16)
        for copy in hop(slot, p, odd):
            copy.start()

    @pl.when(core != FIRST)
    def _():
        give()
        pl.semaphore_wait(gate, 1)

    shares = [share_of(group_of(step, core)) for step in range(ring)]
    @pl.when(core != FIRST)
    def _():
        slabs_in(1 - FIRST)

    def far(q, carry):
        for odd in range(2):
            p = 2 * q + odd
            pair_copy(0, p).wait_recv()
            encode(0, p, odd, pair_sum(2, piece_of(p)))
        return carry

    lax.fori_loop(0, pieces // 2, far, 0)

    def combine(q, carry):
        for odd in range(2):
            p = 2 * q + odd
            pair_copy(1, p).wait_recv()
            slot, step = ((2, 3), (1, 1))[odd]
            encode(slot, p, odd, pair_sum(step, piece_of(p)))
            slot, step = ((1, 1), (2, 3))[odd]
            landed(0, p)
            encode(slot, p, odd, pair_sum(step, piece_of(p)) + decode(0, p, piece_of(p), piece))
        return carry

    lax.fori_loop(0, pieces // 2, combine, 0)

    pl.semaphore_wait(ready.at[0], len(near))
    greet(ready.at[1], near)
    @pl.when(core == FIRST)
    def _():
        slabs_in(1 - FIRST)
        give()

    for copy in small[1:]:
        copy.wait()
    params = [
        pltpu.make_async_copy(src.at[0], dst, param_sem.at[i])
        for i, (src, dst) in enumerate(
            ((mom_hbm, mom), (second_hbm, second), (weight_hbm, weight))
        )
    ]
    for copy in params:
        copy.start()


    shape = (rows, layer.shape[1])
    lane = lax.broadcasted_iota(jnp.int32, shape, 1)
    slot = lane // rows
    diagonal = lane % rows == lax.broadcasted_iota(jnp.int32, shape, 0)

    def halves(value):
        high = value.astype(jnp.bfloat16).astype(jnp.float32)
        return high, value - high

    def place(h, carry):
        block = jnp.zeros(shape, jnp.float32)
        for f in range(5):
            high, low = halves(jnp.full(shape, in_weight[f, h]))
            whole = slot == f
            if f < 4:
                whole = jnp.logical_or(whole, slot == 5 + f)
            block = jnp.where(whole, high, jnp.where(slot == 9 + f, low, block))
        block = jnp.where(diagonal, block, 0.0)
        layer[pl.ds(pl.multiple_of(h * rows, rows), rows), :] = block.astype(jnp.bfloat16)
        return carry

    lax.fori_loop(0, units, place, 0)
    pl.semaphore_wait(ready.at[1], len(near))
    greet(ready.at[2], near)
    for copy in params:
        copy.wait()

    def moments(p, carry):
        for slot in (1, 2):
            landed(slot, p)

        @pl.when(jnp.logical_and(core == FIRST, p == GATE_PIECE))
        def _():
            pl.semaphore_signal(
                gate,
                inc=1,
                device_id={"ep": partner},
                device_id_type=pl.DeviceIdType.MESH,
            )

        def one(i, inner):
            grad_acc, mom_acc = inner
            cols = cols_of(p, i)
            total = pair_sum(0, cols) + decode(1, p, cols, narrow) + decode(2, p, cols, narrow)
            mom_next = MOMENTUM_DECAY * mom[:, cols] + (1.0 - MOMENTUM_DECAY) * total
            gradient[:, cols] = total
            mom[:, cols] = mom_next
            second[:, cols] = (
                SECOND_DECAY * second[:, cols] + (1.0 - SECOND_DECAY) * total * total
            )
            return grad_acc + total * total, mom_acc + mom_next * mom_next

        return lax.fori_loop(0, piece // narrow, one, carry, unroll=True)

    zero = jnp.zeros((rows, narrow), jnp.float32)
    grad_acc, mom_acc = lax.fori_loop(0, pieces, moments, (zero, zero))

    def to_lanes(acc):
        acc = jnp.sum(acc, axis=0, keepdims=True)
        return sum(acc[:, j : j + LANES] for j in range(0, narrow, LANES))

    pl.semaphore_wait(ready.at[2], len(near))
    sums[me, 0:1, :] = to_lanes(grad_acc)
    sums[me, 1:2, :] = to_lanes(mom_acc)
    def hops(offset):
        return min(offset, SIDE - offset)

    offsets = sorted(
        ((up, along) for up in range(SIDE) for along in range(SIDE)),
        key=lambda pair: -hops(pair[0]) - hops(pair[1]),
    )
    for up, along in offsets[:-1]:
        peer = (z + up) % SIDE * SIDE + (x + along) % SIDE
        remote(sums.at[me], sums.at[me], sum_send, sum_recv, "fs", peer).start()
    others = sums.at[pl.ds(0, shards - 1)]
    all_sums = remote(others, others, sum_send, sum_recv, "fs", (me + 1) % shards)
    all_sums.wait_recv()

    entries = rows * columns * shards
    totals = sums[0]
    for s in range(1, shards):
        totals = totals + sums[s]
    mean = jnp.broadcast_to(jnp.sum(totals, axis=1, keepdims=True) / entries, (2, LANES)) + NORM_EPS
    inverse = lax.rsqrt(mean)
    log_mom = 0.5 * jnp.log(mean[1:2, :])
    tail = pl.ds(shape[1] - LANES, LANES)
    biased = slot[:, -LANES:] >= 14
    first = slot[:, -LANES:] == 14
    ends = diagonal[:, -LANES:]

    def settle(h, carry):
        value = in_bias[h] + in_weight[5, h] * log_mom
        high, low = halves(jnp.broadcast_to(value, ends.shape))
        span = pl.ds(pl.multiple_of(h * rows, rows), rows)
        block = jnp.where(ends, jnp.where(first, high, low), 0.0)
        kept = layer[span, tail].astype(jnp.float32)
        layer[span, tail] = jnp.where(biased, block, kept).astype(jnp.bfloat16)
        return carry

    lax.fori_loop(0, units, settle, 0, unroll=True)

    chunks = pass_recv.shape[1]
    width = columns // chunks
    tile = tile_width(width, TILE)
    inv_grad = spread_lanes(inverse[0:1, :], tile)
    inv_mom = spread_lanes(inverse[1:2, :], tile)

    def learned_step(cols):
        grad = gradient[:, cols]
        mom_next = mom[:, cols]
        narrow_old = weight[:, cols]
        inv_root = lax.rsqrt(second[:, cols] + ROOT_EPS)
        highs, lows = [], []
        for value in (
            grad * inv_grad,
            mom_next * inv_mom,
            mom_next * inv_root,
            grad * inv_root,
        ):
            high = value.astype(jnp.bfloat16)
            highs.append(high)
            lows.append((value - high.astype(jnp.float32)).astype(jnp.bfloat16))
        highs.append(narrow_old)
        ones = jnp.ones(grad.shape, jnp.bfloat16)
        features = jnp.concatenate(highs + lows + highs + [ones, ones], axis=0)
        hidden = jnp.dot(layer[...], features, preferred_element_type=jnp.float32)
        directions = [jnp.full(grad.shape, out_bias[0]), jnp.zeros(grad.shape, jnp.float32)]
        magnitudes = [jnp.full(grad.shape, out_bias[1]), jnp.zeros(grad.shape, jnp.float32)]
        for h in range(units):
            active = jnp.maximum(hidden[h * rows : (h + 1) * rows, :], 0.0)
            side = 2 * h // units
            directions[side] = directions[side] + active * out_weight[0, h]
            magnitudes[side] = magnitudes[side] + active * out_weight[1, h]
        direction = directions[0] + directions[1]
        magnitude = magnitudes[0] + magnitudes[1]
        update = STEP_SCALE * direction * jnp.exp(EXP_SCALE * magnitude)
        return (narrow_old.astype(jnp.float32) - update).astype(jnp.bfloat16)

    def rows_of(source):
        return pl.ds(pl.multiple_of(source * rows, rows), rows)

    def block(source, k):
        return gathered.at[rows_of(source), pl.ds(pl.multiple_of(k * width, width), width)]

    def route(k):
        swap = k % 2
        turn = 1 - 2 * (k // 2 % 2)

        def at(first, after):
            up = (z + 2 * SIDE + first * swap + after * (1 - swap)) % SIDE
            along = (x + 2 * SIDE + first * (1 - swap) + after * swap) % SIDE
            return up * SIDE + along

        return at, turn

    def send(source, k, role, recv, peer):
        remote(block(source, k), block(source, k), row_send.at[role], recv, "fs", peer).start()

    def spread(source, k, role, at, way):
        send(source, k, role, pass_recv.at[role, k], at(0, way))
        send(source, k, role, last_recv, at(0, -way))

    def arrive(stage, k, count):
        part = gathered.at[pl.ds(0, count * rows), pl.ds(pl.multiple_of(k * width, width), width)]
        remote(part, part, row_send.at[0], pass_recv.at[stage, k], "fs", me).wait_recv()

    def pass_on(k, role, first):
        at, turn = route(k)
        way = turn if first % 2 == 0 else -turn
        source = at(first * turn, -way)
        send(source, k, role, last_recv, at(0, way))

    def own(k):
        at, turn = route(k)
        send(me, k, 0, pass_recv.at[0, k], at(turn, 0))
        send(me, k, 0, pass_recv.at[0, k], at(-turn, 0))
        spread(me, k, 0, at, turn)

    def relay_one(k):
        at, turn = route(k)
        arrive(0, k, 3)
        source = at(-turn, 0)
        send(source, k, 1, pass_recv.at[1, k], at(turn, 0))
        spread(source, k, 1, at, -turn)
        spread(at(turn, 0), k, 1, at, -turn)
        pass_on(k, 1, 0)

    def relay_two(k):
        at, turn = route(k)
        arrive(1, k, 3)
        spread(at(2, 0), k, 2, at, turn)
        pass_on(k, 2, -1)
        pass_on(k, 2, 1)

    def relay_three(k):
        arrive(2, k, 1)
        pass_on(k, 3, 2)

    def turn_of(t, carry):
        for lag, relay in ((LAG_ONE, relay_one), (LAG_TWO, relay_two), (LAG_THREE, relay_three)):
            k = t - lag

            @pl.when(jnp.logical_and(k >= 0, k < chunks))
            def _(k=k, relay=relay):
                relay(k)

        @pl.when(t < chunks)
        def _():
            def one(i, inner):
                cols = pl.ds(pl.multiple_of(t * width + i * tile, tile), tile)
                gathered[rows_of(me), cols] = learned_step(cols)
                return inner

            lax.fori_loop(0, width // tile, one, 0)
            own(t)

        return carry

    lax.fori_loop(0, chunks + LAG_THREE, turn_of, 0)

    for part in range(2):
        slots = (pl.ds(0, 1), pl.ds(1, ring - 1))[part]
        remote(
            pair_out.at[slots], pair_in.at[slots], pair_send.at[part], pair_recv.at[part, 0], "ep", partner
        ).wait_send()
    for slot in range(3):
        remote(
            ring_out.at[slot], ring_in.at[slot], ring_send.at[slot], ring_recv.at[slot, 0], "ep", partner
        ).wait_send()
        remote(
            scale_out.at[slot], scale_in.at[slot], scale_send.at[slot], ring_recv.at[slot, 0], "ep", partner
        ).wait_send()
    all_sums.wait_send()
    part = gathered.at[pl.ds(0, 8 * rows), :]
    remote(part, part, row_send.at[0], last_recv, "fs", me).wait_recv()
    for role, number in enumerate((4, 6, 4, 1)):
        part = gathered.at[pl.ds(0, number * rows), :]
        remote(
            part, part, row_send.at[role], last_recv, "fs", (me + 1) % shards
        ).wait_send()


def store(gathered, mom, second, gathered_hbm, mom_hbm, second_hbm, sems):
    height = gathered.shape[1] // STORES
    copies = [
        pltpu.make_async_copy(
            gathered.at[:, pl.ds(i * height, height), :],
            gathered_hbm.at[:, pl.ds(i * height, height), :],
            sems.at[i],
        )
        for i in range(STORES)
    ]
    copies.append(pltpu.make_async_copy(mom, mom_hbm, sems.at[STORES]))
    copies.append(pltpu.make_async_copy(second, second_hbm, sems.at[STORES + 1]))
    for copy in copies:
        copy.start()
    for copy in copies:
        copy.wait()


def per_device(groups, grads, counts, weight, mom, second, in_weight, in_bias, out_weight, out_bias):
    rows, columns = mom.shape[1], mom.shape[2]
    ring = groups // CORES
    shards = SIDE * SIDE
    pieces = PIECES
    chunks = CHUNKS
    hbm = pl.BlockSpec(memory_space=pltpu.HBM)
    vmem = pl.BlockSpec(memory_space=pltpu.VMEM)
    results = pl.pallas_call(
        functools.partial(kernel, ring),
        out_shape=(
            pltpu.VMEM((1, rows * shards, columns), jnp.bfloat16),
            pltpu.VMEM(mom.shape, jnp.float32),
            pltpu.VMEM(second.shape, jnp.float32),
        ),
        in_specs=[hbm] * 9,
        out_specs=(vmem, vmem, vmem),
        scratch_shapes=[
            pltpu.SMEM(counts.shape, jnp.int32),
            pltpu.SMEM(in_weight.shape, jnp.float32),
            pltpu.SMEM(in_bias.shape, jnp.float32),
            pltpu.SMEM(out_weight.shape[::-1], jnp.float32),
            pltpu.SMEM(out_bias.shape, jnp.float32),
            pltpu.VMEM((CORES, ring, rows, columns), jnp.bfloat16),
            pltpu.VMEM((rows, columns), jnp.bfloat16),
            pltpu.VMEM((ring, rows, columns), jnp.bfloat16),
            pltpu.VMEM((ring, rows, columns), jnp.bfloat16),
            pltpu.VMEM((ring - 1, rows, columns), jnp.int16),
            pltpu.VMEM((ring - 1, rows, columns), jnp.int16),
            pltpu.VMEM((ring - 1, pieces, 1, LANES), jnp.float32),
            pltpu.VMEM((ring - 1, pieces, 1, LANES), jnp.float32),
            pltpu.VMEM((rows, columns), jnp.float32),
            pltpu.VMEM((shards, 2, LANES), jnp.float32),
            pltpu.VMEM((in_bias.shape[0] * rows, 16 * rows), jnp.bfloat16),
            pltpu.VMEM((rows * columns // pieces * 2 // (4 * LANES) + 1, LANES), jnp.float32),
            pltpu.SemaphoreType.DMA((5,)),
            pltpu.SemaphoreType.DMA((CORES,)),
            pltpu.SemaphoreType.DMA((3,)),
            pltpu.SemaphoreType.DMA((2,)),
            pltpu.SemaphoreType.DMA((2, pieces)),
            pltpu.SemaphoreType.DMA((ring - 1,)),
            pltpu.SemaphoreType.DMA((ring - 1, pieces)),
            pltpu.SemaphoreType.DMA((ring - 1,)),
            pltpu.SemaphoreType.REGULAR,
            pltpu.SemaphoreType.REGULAR((3,)),
            pltpu.SemaphoreType.DMA,
            pltpu.SemaphoreType.DMA,
            pltpu.SemaphoreType.DMA((4,)),
            pltpu.SemaphoreType.DMA((3, chunks)),
            pltpu.SemaphoreType.DMA,
        ],
        compiler_params=pltpu.CompilerParams(
            collective_id=0, has_side_effects=True, vmem_limit_bytes=VMEM_BYTES
        ),
        name="learned_update",
    )(counts, in_weight, in_bias, out_weight.T, out_bias, grads, weight, mom, second)
    return pl.pallas_call(
        store,
        out_shape=[jax.ShapeDtypeStruct(r.shape, r.dtype) for r in results],
        in_specs=[vmem] * 3,
        out_specs=[hbm] * 3,
        scratch_shapes=[pltpu.SemaphoreType.DMA((STORES + 2,))],
        compiler_params=pltpu.CompilerParams(vmem_limit_bytes=1024 * 1024),
        name="store_results",
    )(*results)


def solution(mesh):
    in_specs = (
        P("ep", None, "fs", None),
        P(),
        P("ep", "fs", None),
        P("ep", "fs", None),
        P("ep", "fs", None),
        P(),
        P(),
        P(),
        P(),
    )
    out_specs = (P("ep", None, None), P("ep", "fs", None), P("ep", "fs", None))
    body = functools.partial(per_device, mesh.shape["ep"])
    return jax.shard_map(
        body, mesh=mesh, in_specs=in_specs, out_specs=out_specs, check_vma=False
    )
```

```python
import functools

import jax
import jax.numpy as jnp
from jax import lax
from jax.experimental import pallas as pl
from jax.experimental.pallas import tpu as pltpu
from jax.sharding import PartitionSpec as P

MOMENTUM_DECAY = 0.9
SECOND_DECAY = 0.99
NORM_EPS = 1e-06
ROOT_EPS = 1e-08
STEP_SCALE = 0.2
EXP_SCALE = 0.5
LANES = 128
CORES = 2
SIDE = 4
CHUNKS = 16
PIECES = 8
LAG_ONE = 6
LAG_TWO = 11
LAG_THREE = 16
GATE_PIECE = 6
EARLY = 3
FIRST = 1
ORDER = (2, 1, 3, 0)
CODES = 32767.0
TINY = 1e-30
TILE = 896
STORES = 4
VMEM_BYTES = 67043328 - 9175040


def largest_divisor(number, most):
    return max(d for d in range(1, most + 1) if number % d == 0)


def tile_width(columns, most):
    return LANES * largest_divisor(columns // LANES, most // LANES)


def remote(src, dst, send_sem, recv_sem, axis, peer):
    return pltpu.make_async_remote_copy(
        src_ref=src,
        dst_ref=dst,
        send_sem=send_sem,
        recv_sem=recv_sem,
        device_id={axis: peer},
        device_id_type=pl.DeviceIdType.MESH,
    )


def kernel(
    ring,
    counts_hbm,
    in_weight_hbm,
    in_bias_hbm,
    out_weight_hbm,
    out_bias_hbm,
    grads_hbm,
    weight_hbm,
    mom_hbm,
    second_hbm,
    gathered_out,
    mom_out,
    second_out,
    counts,
    in_weight,
    in_bias,
    out_weight,
    out_bias,
    grads,
    weight,
    pair_out,
    pair_in,
    ring_out,
    ring_in,
    scale_out,
    scale_in,
    gradient,
    sums,
    layer,
    tally,
    small_sem,
    slab_sem,
    param_sem,
    pair_send,
    pair_recv,
    ring_send,
    ring_recv,
    scale_send,
    gate,
    ready,
    sum_send,
    sum_recv,
    row_send,
    pass_recv,
    last_recv,
):
    gathered = gathered_out.at[0]
    mom = mom_out.at[0]
    second = second_out.at[0]
    groups = ring * CORES
    shards = SIDE * SIDE
    rows, columns = gradient.shape
    units = in_bias.shape[0]
    me_group = lax.axis_index("ep")
    me = lax.axis_index("fs")
    y = me_group // CORES
    core = me_group % CORES
    partner = y * CORES + 1 - core
    z = me // SIDE
    x = me % SIDE

    def group_of(step, which):
        return (y + step) % ring * CORES + which

    small = [
        pltpu.make_async_copy(src, dst, small_sem.at[i])
        for i, (src, dst) in enumerate(
            (
                (counts_hbm, counts),
                (in_weight_hbm, in_weight),
                (in_bias_hbm, in_bias),
                (out_weight_hbm, out_weight),
                (out_bias_hbm, out_bias),
            )
        )
    ]
    for copy in small:
        copy.start()

    def slab(which, step):
        return pltpu.make_async_copy(
            grads_hbm.at[0, group_of(step, which)],
            grads.at[which, step],
            slab_sem.at[which],
        )

    def slabs_in(which):
        pltpu.make_async_copy(
            grads_hbm.at[0, pl.ds(0, ring)], grads.at[which], slab_sem.at[which]
        ).wait()

    for which in (FIRST, 1 - FIRST):
        for step in ORDER:
            slab(which, step).start()
    barrier = pltpu.get_barrier_semaphore()
    near = [
        {"fs": up * SIDE + along}
        for up, along in (
            (z, (x + 1) % SIDE),
            (z, (x + SIDE - 1) % SIDE),
            ((z + 1) % SIDE, x),
            ((z + SIDE - 1) % SIDE, x),
        )
    ]

    def greet(semaphore, peers):
        for peer in peers:
            pl.semaphore_signal(
                semaphore, inc=1, device_id=peer, device_id_type=pl.DeviceIdType.MESH
            )

    beside = [{"ep": peer} for peer in (partner, group_of(1, core), group_of(ring - 1, core))]
    greet(barrier, beside + near)
    small[0].wait()

    pieces = ring_recv.shape[1]
    piece = columns // pieces
    narrow = tile_width(piece, 512)

    def cols_of(p, i):
        return pl.ds(pl.multiple_of(p * piece + i * narrow, narrow), narrow)

    def piece_of(p):
        return pl.ds(pl.multiple_of(p * piece, piece), piece)

    def share_of(expert):
        total = counts[0, expert]
        for s in range(1, groups):
            total = total + counts[s, expert]
        mine = jnp.full((1, LANES), counts[me_group, expert].astype(jnp.float32))
        return (mine / jnp.full((1, LANES), total.astype(jnp.float32)))[:, :1]

    def weighted(share, which, step, cols):
        value = share * grads[which, step, :, cols].astype(jnp.float32)
        return value.astype(jnp.bfloat16)

    slabs_in(FIRST)
    pl.semaphore_wait(barrier, len(beside) + len(near))
    greet(ready.at[0], near)

    def pair_copy(part, p):
        slots = (pl.ds(0, 1), pl.ds(1, ring - 1))[part]
        return remote(
            pair_out.at[slots, :, piece_of(p)],
            pair_in.at[slots, :, piece_of(p)],
            pair_send.at[part],
            pair_recv.at[part, p],
            "ep",
            partner,
        )

    def give():
        shares = [share_of(group_of(step, 1 - core)) for step in range(ring)]
        for part, steps in enumerate((ORDER[:1], ORDER[1:])):

            def body(p, carry, part=part, steps=steps):
                for step in steps:
                    pair_out[ORDER.index(step), :, piece_of(p)] = weighted(
                        shares[step], 1 - core, step, piece_of(p)
                    )
                pair_copy(part, p).start()
                return carry

            lax.fori_loop(0, pieces, body, 0)

    def hop(slot, p, odd=0):
        step = (1 - 2 * odd, 1, -1)[slot]
        peer = group_of(step + ring, core)
        codes = remote(
            ring_out.at[slot, :, piece_of(p)],
            ring_in.at[slot, :, piece_of(p)],
            ring_send.at[slot],
            ring_recv.at[slot, p],
            "ep",
            peer,
        )
        scale = remote(
            scale_out.at[slot, p],
            scale_in.at[slot, p],
            scale_send.at[slot],
            ring_recv.at[slot, p],
            "ep",
            peer,
        )
        return codes, scale

    def landed(slot, p):
        remote(tally, tally, ring_send.at[slot], ring_recv.at[slot, p], "ep", partner).wait_recv()

    def spread_lanes(row, width):
        return jnp.concatenate([row] * (width // LANES), axis=1)

    def pair_sum(step, cols):
        total = weighted(shares[step], core, step, cols).astype(jnp.float32)
        return total + pair_in[ORDER.index(step), :, cols].astype(jnp.float32)

    def decode(slot, p, cols, width):
        codes = ring_in[slot, :, cols].astype(jnp.int32).astype(jnp.float32)
        return codes * spread_lanes(scale_in[slot, p], width)

    def encode(slot, p, odd, total):
        most = jnp.max(jnp.abs(total), axis=0, keepdims=True)
        parts = [most[:, j : j + LANES] for j in range(0, piece, LANES)]
        most = jnp.maximum(functools.reduce(jnp.maximum, parts), TINY)
        scale_out[slot, p] = most * (1.0 / CODES)
        codes = lax.round(
            total * spread_lanes(CODES / most, piece), lax.RoundingMethod.TO_NEAREST_EVEN
        )
        ring_out[slot, :, piece_of(p)] = codes.astype(jnp.int32).astype(jnp.int16)
        for copy in hop(slot, p, odd):
            copy.start()

    @pl.when(core != FIRST)
    def _():
        give()
        pl.semaphore_wait(gate, 1)

    shares = [share_of(group_of(step, core)) for step in range(ring)]
    @pl.when(core != FIRST)
    def _():
        slabs_in(1 - FIRST)

    def far(q, carry):
        for odd in range(2):
            p = 2 * q + odd
            pair_copy(0, p).wait_recv()
            encode(0, p, odd, pair_sum(2, piece_of(p)))
        return carry

    lax.fori_loop(0, pieces // 2, far, 0)

    def combine(q, carry):
        for odd in range(2):
            p = 2 * q + odd
            pair_copy(1, p).wait_recv()
            slot, step = ((2, 3), (1, 1))[odd]
            encode(slot, p, odd, pair_sum(step, piece_of(p)))
            slot, step = ((1, 1), (2, 3))[odd]
            landed(0, p)
            encode(slot, p, odd, pair_sum(step, piece_of(p)) + decode(0, p, piece_of(p), piece))
        return carry

    lax.fori_loop(0, pieces // 2, combine, 0)

    pl.semaphore_wait(ready.at[0], len(near))
    greet(ready.at[1], near)
    @pl.when(core == FIRST)
    def _():
        slabs_in(1 - FIRST)
        give()

    for copy in small[1:]:
        copy.wait()
    params = [
        pltpu.make_async_copy(src.at[0], dst, param_sem.at[i])
        for i, (src, dst) in enumerate(
            ((mom_hbm, mom), (second_hbm, second), (weight_hbm, weight))
        )
    ]
    for copy in params:
        copy.start()


    shape = (rows, layer.shape[1])
    lane = lax.broadcasted_iota(jnp.int32, shape, 1)
    slot = lane // rows
    diagonal = lane % rows == lax.broadcasted_iota(jnp.int32, shape, 0)

    def halves(value):
        high = value.astype(jnp.bfloat16).astype(jnp.float32)
        return high, value - high

    def place(h, carry):
        block = jnp.zeros(shape, jnp.float32)
        for f in range(5):
            high, low = halves(jnp.full(shape, in_weight[f, h]))
            whole = slot == f
            if f < 4:
                whole = jnp.logical_or(whole, slot == 5 + f)
            block = jnp.where(whole, high, jnp.where(slot == 9 + f, low, block))
        block = jnp.where(diagonal, block, 0.0)
        layer[pl.ds(pl.multiple_of(h * rows, rows), rows), :] = block.astype(jnp.bfloat16)
        return carry

    lax.fori_loop(0, units, place, 0)
    pl.semaphore_wait(ready.at[1], len(near))
    greet(ready.at[2], near)
    for copy in params:
        copy.wait()

    def moments(p, carry):
        for slot in (1, 2):
            landed(slot, p)

        @pl.when(jnp.logical_and(core == FIRST, p == GATE_PIECE))
        def _():
            pl.semaphore_signal(
                gate,
                inc=1,
                device_id={"ep": partner},
                device_id_type=pl.DeviceIdType.MESH,
            )

        def one(i, inner):
            grad_acc, mom_acc = inner
            cols = cols_of(p, i)
            total = pair_sum(0, cols) + decode(1, p, cols, narrow) + decode(2, p, cols, narrow)
            mom_next = MOMENTUM_DECAY * mom[:, cols] + (1.0 - MOMENTUM_DECAY) * total
            gradient[:, cols] = total
            mom[:, cols] = mom_next
            second[:, cols] = (
                SECOND_DECAY * second[:, cols] + (1.0 - SECOND_DECAY) * total * total
            )
            return grad_acc + total * total, mom_acc + mom_next * mom_next

        return lax.fori_loop(0, piece // narrow, one, carry, unroll=True)

    zero = jnp.zeros((rows, narrow), jnp.float32)
    grad_acc, mom_acc = lax.fori_loop(0, pieces, moments, (zero, zero))

    def to_lanes(acc):
        acc = jnp.sum(acc, axis=0, keepdims=True)
        return sum(acc[:, j : j + LANES] for j in range(0, narrow, LANES))

    pl.semaphore_wait(ready.at[2], len(near))
    sums[me, 0:1, :] = to_lanes(grad_acc)
    sums[me, 1:2, :] = to_lanes(mom_acc)
    def hops(offset):
        return min(offset, SIDE - offset)

    offsets = sorted(
        ((up, along) for up in range(SIDE) for along in range(SIDE)),
        key=lambda pair: -hops(pair[0]) - hops(pair[1]),
    )
    for up, along in offsets[:-1]:
        peer = (z + up) % SIDE * SIDE + (x + along) % SIDE
        remote(sums.at[me], sums.at[me], sum_send, sum_recv, "fs", peer).start()
    others = sums.at[pl.ds(0, shards - 1)]
    all_sums = remote(others, others, sum_send, sum_recv, "fs", (me + 1) % shards)
    all_sums.wait_recv()

    entries = rows * columns * shards
    totals = sums[0]
    for s in range(1, shards):
        totals = totals + sums[s]
    mean = jnp.broadcast_to(jnp.sum(totals, axis=1, keepdims=True) / entries, (2, LANES)) + NORM_EPS
    inverse = lax.rsqrt(mean)
    log_mom = 0.5 * jnp.log(mean[1:2, :])
    tail = pl.ds(shape[1] - LANES, LANES)
    biased = slot[:, -LANES:] >= 14
    first = slot[:, -LANES:] == 14
    ends = diagonal[:, -LANES:]

    def settle(h, carry):
        value = in_bias[h] + in_weight[5, h] * log_mom
        high, low = halves(jnp.broadcast_to(value, ends.shape))
        span = pl.ds(pl.multiple_of(h * rows, rows), rows)
        block = jnp.where(ends, jnp.where(first, high, low), 0.0)
        kept = layer[span, tail].astype(jnp.float32)
        layer[span, tail] = jnp.where(biased, block, kept).astype(jnp.bfloat16)
        return carry

    lax.fori_loop(0, units, settle, 0, unroll=True)

    chunks = pass_recv.shape[1]
    width = columns // chunks
    tile = tile_width(width, TILE)
    inv_grad = spread_lanes(inverse[0:1, :], tile)
    inv_mom = spread_lanes(inverse[1:2, :], tile)

    def learned_step(cols):
        grad = gradient[:, cols]
        mom_next = mom[:, cols]
        narrow_old = weight[:, cols]
        inv_root = lax.rsqrt(second[:, cols] + ROOT_EPS)
        highs, lows = [], []
        for value in (
            grad * inv_grad,
            mom_next * inv_mom,
            mom_next * inv_root,
            grad * inv_root,
        ):
            high = value.astype(jnp.bfloat16)
            highs.append(high)
            lows.append((value - high.astype(jnp.float32)).astype(jnp.bfloat16))
        highs.append(narrow_old)
        ones = jnp.ones(grad.shape, jnp.bfloat16)
        features = jnp.concatenate(highs + lows + highs + [ones, ones], axis=0)
        hidden = jnp.dot(layer[...], features, preferred_element_type=jnp.float32)
        directions = [jnp.full(grad.shape, out_bias[0]), jnp.zeros(grad.shape, jnp.float32)]
        magnitudes = [jnp.full(grad.shape, out_bias[1]), jnp.zeros(grad.shape, jnp.float32)]
        for h in range(units):
            active = jnp.maximum(hidden[h * rows : (h + 1) * rows, :], 0.0)
            side = 2 * h // units
            directions[side] = directions[side] + active * out_weight[0, h]
            magnitudes[side] = magnitudes[side] + active * out_weight[1, h]
        direction = directions[0] + directions[1]
        magnitude = magnitudes[0] + magnitudes[1]
        update = STEP_SCALE * direction * jnp.exp(EXP_SCALE * magnitude)
        return (narrow_old.astype(jnp.float32) - update).astype(jnp.bfloat16)

    def rows_of(source):
        return pl.ds(pl.multiple_of(source * rows, rows), rows)

    def block(source, k):
        return gathered.at[rows_of(source), pl.ds(pl.multiple_of(k * width, width), width)]

    def route(k):
        swap = k % 2
        turn = 1 - 2 * (k // 2 % 2)

        def at(first, after):
            up = (z + 2 * SIDE + first * swap + after * (1 - swap)) % SIDE
            along = (x + 2 * SIDE + first * (1 - swap) + after * swap) % SIDE
            return up * SIDE + along

        return at, turn

    def send(source, k, role, recv, peer):
        remote(block(source, k), block(source, k), row_send.at[role], recv, "fs", peer).start()

    def spread(source, k, role, at, way):
        send(source, k, role, pass_recv.at[role, k], at(0, way))
        send(source, k, role, last_recv, at(0, -way))

    def arrive(stage, k, count):
        part = gathered.at[pl.ds(0, count * rows), pl.ds(pl.multiple_of(k * width, width), width)]
        remote(part, part, row_send.at[0], pass_recv.at[stage, k], "fs", me).wait_recv()

    def pass_on(k, role, first):
        at, turn = route(k)
        way = turn if first % 2 == 0 else -turn
        source = at(first * turn, -way)
        send(source, k, role, last_recv, at(0, way))

    def own(k):
        at, turn = route(k)
        send(me, k, 0, pass_recv.at[0, k], at(turn, 0))
        send(me, k, 0, pass_recv.at[0, k], at(-turn, 0))
        spread(me, k, 0, at, turn)

    def relay_one(k):
        at, turn = route(k)
        arrive(0, k, 3)
        source = at(-turn, 0)
        send(source, k, 1, pass_recv.at[1, k], at(turn, 0))
        spread(source, k, 1, at, -turn)
        spread(at(turn, 0), k, 1, at, -turn)
        pass_on(k, 1, 0)

    def relay_two(k):
        at, turn = route(k)
        arrive(1, k, 3)
        spread(at(2, 0), k, 2, at, turn)
        pass_on(k, 2, -1)
        pass_on(k, 2, 1)

    def relay_three(k):
        arrive(2, k, 1)
        pass_on(k, 3, 2)

    def turn_of(t, carry):
        for lag, relay in ((LAG_ONE, relay_one), (LAG_TWO, relay_two), (LAG_THREE, relay_three)):
            early = t - lag + 1 < EARLY
            k = t - lag + jnp.where(early, 1, 0)

            @pl.when(jnp.logical_and(k >= jnp.where(early, 0, EARLY), k < chunks))
            def _(k=k, relay=relay):
                relay(k)

        @pl.when(t < chunks)
        def _():
            def one(i, inner):
                cols = pl.ds(pl.multiple_of(t * width + i * tile, tile), tile)
                gathered[rows_of(me), cols] = learned_step(cols)
                return inner

            lax.fori_loop(0, width // tile, one, 0)
            own(t)

        return carry

    lax.fori_loop(0, chunks + LAG_THREE, turn_of, 0)

    for part in range(2):
        slots = (pl.ds(0, 1), pl.ds(1, ring - 1))[part]
        remote(
            pair_out.at[slots], pair_in.at[slots], pair_send.at[part], pair_recv.at[part, 0], "ep", partner
        ).wait_send()
    for slot in range(3):
        remote(
            ring_out.at[slot], ring_in.at[slot], ring_send.at[slot], ring_recv.at[slot, 0], "ep", partner
        ).wait_send()
        remote(
            scale_out.at[slot], scale_in.at[slot], scale_send.at[slot], ring_recv.at[slot, 0], "ep", partner
        ).wait_send()
    all_sums.wait_send()
    part = gathered.at[pl.ds(0, 8 * rows), :]
    remote(part, part, row_send.at[0], last_recv, "fs", me).wait_recv()
    for role, number in enumerate((4, 6, 4, 1)):
        part = gathered.at[pl.ds(0, number * rows), :]
        remote(
            part, part, row_send.at[role], last_recv, "fs", (me + 1) % shards
        ).wait_send()


def store(gathered, mom, second, gathered_hbm, mom_hbm, second_hbm, sems):
    height = gathered.shape[1] // STORES
    copies = [
        pltpu.make_async_copy(
            gathered.at[:, pl.ds(i * height, height), :],
            gathered_hbm.at[:, pl.ds(i * height, height), :],
            sems.at[i],
        )
        for i in range(STORES)
    ]
    copies.append(pltpu.make_async_copy(mom, mom_hbm, sems.at[STORES]))
    copies.append(pltpu.make_async_copy(second, second_hbm, sems.at[STORES + 1]))
    for copy in copies:
        copy.start()
    for copy in copies:
        copy.wait()


def per_device(groups, grads, counts, weight, mom, second, in_weight, in_bias, out_weight, out_bias):
    rows, columns = mom.shape[1], mom.shape[2]
    ring = groups // CORES
    shards = SIDE * SIDE
    pieces = PIECES
    chunks = CHUNKS
    hbm = pl.BlockSpec(memory_space=pltpu.HBM)
    vmem = pl.BlockSpec(memory_space=pltpu.VMEM)
    results = pl.pallas_call(
        functools.partial(kernel, ring),
        out_shape=(
            pltpu.VMEM((1, rows * shards, columns), jnp.bfloat16),
            pltpu.VMEM(mom.shape, jnp.float32),
            pltpu.VMEM(second.shape, jnp.float32),
        ),
        in_specs=[hbm] * 9,
        out_specs=(vmem, vmem, vmem),
        scratch_shapes=[
            pltpu.SMEM(counts.shape, jnp.int32),
            pltpu.SMEM(in_weight.shape, jnp.float32),
            pltpu.SMEM(in_bias.shape, jnp.float32),
            pltpu.SMEM(out_weight.shape[::-1], jnp.float32),
            pltpu.SMEM(out_bias.shape, jnp.float32),
            pltpu.VMEM((CORES, ring, rows, columns), jnp.bfloat16),
            pltpu.VMEM((rows, columns), jnp.bfloat16),
            pltpu.VMEM((ring, rows, columns), jnp.bfloat16),
            pltpu.VMEM((ring, rows, columns), jnp.bfloat16),
            pltpu.VMEM((ring - 1, rows, columns), jnp.int16),
            pltpu.VMEM((ring - 1, rows, columns), jnp.int16),
            pltpu.VMEM((ring - 1, pieces, 1, LANES), jnp.float32),
            pltpu.VMEM((ring - 1, pieces, 1, LANES), jnp.float32),
            pltpu.VMEM((rows, columns), jnp.float32),
            pltpu.VMEM((shards, 2, LANES), jnp.float32),
            pltpu.VMEM((in_bias.shape[0] * rows, 16 * rows), jnp.bfloat16),
            pltpu.VMEM((rows * columns // pieces * 2 // (4 * LANES) + 1, LANES), jnp.float32),
            pltpu.SemaphoreType.DMA((5,)),
            pltpu.SemaphoreType.DMA((CORES,)),
            pltpu.SemaphoreType.DMA((3,)),
            pltpu.SemaphoreType.DMA((2,)),
            pltpu.SemaphoreType.DMA((2, pieces)),
            pltpu.SemaphoreType.DMA((ring - 1,)),
            pltpu.SemaphoreType.DMA((ring - 1, pieces)),
            pltpu.SemaphoreType.DMA((ring - 1,)),
            pltpu.SemaphoreType.REGULAR,
            pltpu.SemaphoreType.REGULAR((3,)),
            pltpu.SemaphoreType.DMA,
            pltpu.SemaphoreType.DMA,
            pltpu.SemaphoreType.DMA((4,)),
            pltpu.SemaphoreType.DMA((3, chunks)),
            pltpu.SemaphoreType.DMA,
        ],
        compiler_params=pltpu.CompilerParams(
            collective_id=0, has_side_effects=True, vmem_limit_bytes=VMEM_BYTES
        ),
        name="learned_update",
    )(counts, in_weight, in_bias, out_weight.T, out_bias, grads, weight, mom, second)
    return pl.pallas_call(
        store,
        out_shape=[jax.ShapeDtypeStruct(r.shape, r.dtype) for r in results],
        in_specs=[vmem] * 3,
        out_specs=[hbm] * 3,
        scratch_shapes=[pltpu.SemaphoreType.DMA((STORES + 2,))],
        compiler_params=pltpu.CompilerParams(vmem_limit_bytes=1024 * 1024),
        name="store_results",
    )(*results)


def solution(mesh):
    in_specs = (
        P("ep", None, "fs", None),
        P(),
        P("ep", "fs", None),
        P("ep", "fs", None),
        P("ep", "fs", None),
        P(),
        P(),
        P(),
        P(),
    )
    out_specs = (P("ep", None, None), P("ep", "fs", None), P("ep", "fs", None))
    body = functools.partial(per_device, mesh.shape["ep"])
    return jax.shard_map(
        body, mesh=mesh, in_specs=in_specs, out_specs=out_specs, check_vma=False
    )
```

```python
import functools

import jax
import jax.numpy as jnp
from jax import lax
from jax.experimental import pallas as pl
from jax.experimental.pallas import tpu as pltpu
from jax.sharding import PartitionSpec as P

MOMENTUM_DECAY = 0.9
SECOND_DECAY = 0.99
NORM_EPS = 1e-06
ROOT_EPS = 1e-08
STEP_SCALE = 0.2
EXP_SCALE = 0.5
LANES = 128
CORES = 2
SIDE = 4
CHUNKS = 16
PIECES = 8
LAG_ONE = 6
LAG_TWO = 11
LAG_THREE = 16
GATE_PIECE = 6
FIRST = 1
ORDER = (2, 1, 3, 0)
CODES = 32767.0
TINY = 1e-30
TILE = 896
STORES = 4
VMEM_BYTES = 67043328 - 9175040


def largest_divisor(number, most):
    return max(d for d in range(1, most + 1) if number % d == 0)


def tile_width(columns, most):
    return LANES * largest_divisor(columns // LANES, most // LANES)


def remote(src, dst, send_sem, recv_sem, axis, peer):
    return pltpu.make_async_remote_copy(
        src_ref=src,
        dst_ref=dst,
        send_sem=send_sem,
        recv_sem=recv_sem,
        device_id={axis: peer},
        device_id_type=pl.DeviceIdType.MESH,
    )


def kernel(
    ring,
    counts_hbm,
    in_weight_hbm,
    in_bias_hbm,
    out_weight_hbm,
    out_bias_hbm,
    grads_hbm,
    weight_hbm,
    mom_hbm,
    second_hbm,
    gathered_out,
    mom_out,
    second_out,
    counts,
    in_weight,
    in_bias,
    out_weight,
    out_bias,
    grads,
    weight,
    pair_out,
    pair_in,
    ring_out,
    ring_in,
    scale_out,
    scale_in,
    gradient,
    sums,
    layer,
    tally,
    small_sem,
    slab_sem,
    param_sem,
    pair_send,
    pair_recv,
    ring_send,
    ring_recv,
    scale_send,
    gate,
    ready,
    sum_send,
    sum_recv,
    row_send,
    pass_recv,
    last_recv,
):
    gathered = gathered_out.at[0]
    mom = mom_out.at[0]
    second = second_out.at[0]
    groups = ring * CORES
    shards = SIDE * SIDE
    rows, columns = gradient.shape
    units = in_bias.shape[0]
    me_group = lax.axis_index("ep")
    me = lax.axis_index("fs")
    y = me_group // CORES
    core = me_group % CORES
    partner = y * CORES + 1 - core
    z = me // SIDE
    x = me % SIDE

    def group_of(step, which):
        return (y + step) % ring * CORES + which

    small = [
        pltpu.make_async_copy(src, dst, small_sem.at[i])
        for i, (src, dst) in enumerate(
            (
                (counts_hbm, counts),
                (in_weight_hbm, in_weight),
                (in_bias_hbm, in_bias),
                (out_weight_hbm, out_weight),
                (out_bias_hbm, out_bias),
            )
        )
    ]
    for copy in small:
        copy.start()

    def slab(which, step):
        return pltpu.make_async_copy(
            grads_hbm.at[0, group_of(step, which)],
            grads.at[which, step],
            slab_sem.at[which],
        )

    def slabs_in(which):
        pltpu.make_async_copy(
            grads_hbm.at[0, pl.ds(0, ring)], grads.at[which], slab_sem.at[which]
        ).wait()

    for which in (FIRST, 1 - FIRST):
        for step in ORDER:
            slab(which, step).start()
    barrier = pltpu.get_barrier_semaphore()
    near = [
        {"fs": up * SIDE + along}
        for up, along in (
            (z, (x + 1) % SIDE),
            (z, (x + SIDE - 1) % SIDE),
            ((z + 1) % SIDE, x),
            ((z + SIDE - 1) % SIDE, x),
        )
    ]

    def greet(semaphore, peers):
        for peer in peers:
            pl.semaphore_signal(
                semaphore, inc=1, device_id=peer, device_id_type=pl.DeviceIdType.MESH
            )

    beside = [{"ep": peer} for peer in (partner, group_of(1, core), group_of(ring - 1, core))]
    greet(barrier, beside + near)
    small[0].wait()

    pieces = ring_recv.shape[1]
    piece = columns // pieces
    narrow = tile_width(piece, 512)

    def cols_of(p, i):
        return pl.ds(pl.multiple_of(p * piece + i * narrow, narrow), narrow)

    def piece_of(p):
        return pl.ds(pl.multiple_of(p * piece, piece), piece)

    def share_of(expert):
        total = counts[0, expert]
        for s in range(1, groups):
            total = total + counts[s, expert]
        mine = jnp.full((1, LANES), counts[me_group, expert].astype(jnp.float32))
        return (mine / jnp.full((1, LANES), total.astype(jnp.float32)))[:, :1]

    gift_shares = [share_of(group_of(step, 1 - core)) for step in range(ring)]
    shares = [share_of(group_of(step, core)) for step in range(ring)]

    def weighted(share, which, step, cols):
        value = share * grads[which, step, :, cols].astype(jnp.float32)
        return value.astype(jnp.bfloat16)

    slabs_in(FIRST)
    pl.semaphore_wait(barrier, len(beside) + len(near))
    greet(ready.at[0], near)

    def pair_copy(part, p):
        slots = (pl.ds(0, 1), pl.ds(1, ring - 1))[part]
        return remote(
            pair_out.at[slots, :, piece_of(p)],
            pair_in.at[slots, :, piece_of(p)],
            pair_send.at[part],
            pair_recv.at[part, p],
            "ep",
            partner,
        )

    def give():
        for part, steps in enumerate((ORDER[:1], ORDER[1:])):

            def body(p, carry, part=part, steps=steps):
                for step in steps:
                    pair_out[ORDER.index(step), :, piece_of(p)] = weighted(
                        gift_shares[step], 1 - core, step, piece_of(p)
                    )
                pair_copy(part, p).start()
                return carry

            lax.fori_loop(0, pieces, body, 0)

    def hop(slot, p, odd=0):
        step = (1 - 2 * odd, 1, -1)[slot]
        peer = group_of(step + ring, core)
        codes = remote(
            ring_out.at[slot, :, piece_of(p)],
            ring_in.at[slot, :, piece_of(p)],
            ring_send.at[slot],
            ring_recv.at[slot, p],
            "ep",
            peer,
        )
        scale = remote(
            scale_out.at[slot, p],
            scale_in.at[slot, p],
            scale_send.at[slot],
            ring_recv.at[slot, p],
            "ep",
            peer,
        )
        return codes, scale

    def landed(slot, p):
        remote(tally, tally, ring_send.at[slot], ring_recv.at[slot, p], "ep", partner).wait_recv()

    def spread_lanes(row, width):
        return jnp.concatenate([row] * (width // LANES), axis=1)

    def pair_sum(step, cols):
        total = weighted(shares[step], core, step, cols).astype(jnp.float32)
        return total + pair_in[ORDER.index(step), :, cols].astype(jnp.float32)

    def decode(slot, p, cols, width):
        codes = ring_in[slot, :, cols].astype(jnp.int32).astype(jnp.float32)
        return codes * spread_lanes(scale_in[slot, p], width)

    def encode(slot, p, odd, total):
        most = jnp.max(jnp.abs(total), axis=0, keepdims=True)
        parts = [most[:, j : j + LANES] for j in range(0, piece, LANES)]
        most = jnp.maximum(functools.reduce(jnp.maximum, parts), TINY)
        scale_out[slot, p] = most * (1.0 / CODES)
        codes = lax.round(
            total * spread_lanes(CODES / most, piece), lax.RoundingMethod.TO_NEAREST_EVEN
        )
        ring_out[slot, :, piece_of(p)] = codes.astype(jnp.int32).astype(jnp.int16)
        for copy in hop(slot, p, odd):
            copy.start()

    @pl.when(core != FIRST)
    def _():
        give()
        pl.semaphore_wait(gate, 1)

    @pl.when(core != FIRST)
    def _():
        slabs_in(1 - FIRST)

    def far(q, carry):
        for odd in range(2):
            p = 2 * q + odd
            pair_copy(0, p).wait_recv()
            encode(0, p, odd, pair_sum(2, piece_of(p)))
        return carry

    lax.fori_loop(0, pieces // 2, far, 0)

    def combine(q, carry):
        for odd in range(2):
            p = 2 * q + odd
            pair_copy(1, p).wait_recv()
            slot, step = ((2, 3), (1, 1))[odd]
            encode(slot, p, odd, pair_sum(step, piece_of(p)))
            slot, step = ((1, 1), (2, 3))[odd]
            landed(0, p)
            encode(slot, p, odd, pair_sum(step, piece_of(p)) + decode(0, p, piece_of(p), piece))
        return carry

    lax.fori_loop(0, pieces // 2, combine, 0)

    pl.semaphore_wait(ready.at[0], len(near))
    greet(ready.at[1], near)
    @pl.when(core == FIRST)
    def _():
        slabs_in(1 - FIRST)
        give()

    for copy in small[1:]:
        copy.wait()
    params = [
        pltpu.make_async_copy(src.at[0], dst, param_sem.at[i])
        for i, (src, dst) in enumerate(
            ((mom_hbm, mom), (second_hbm, second), (weight_hbm, weight))
        )
    ]
    for copy in params:
        copy.start()


    shape = (rows, layer.shape[1])
    lane = lax.broadcasted_iota(jnp.int32, shape, 1)
    slot = lane // rows
    diagonal = lane % rows == lax.broadcasted_iota(jnp.int32, shape, 0)

    def halves(value):
        high = value.astype(jnp.bfloat16).astype(jnp.float32)
        return high, value - high

    def place(h, carry):
        block = jnp.zeros(shape, jnp.float32)
        for f in range(5):
            high, low = halves(jnp.full(shape, in_weight[f, h]))
            whole = slot == f
            if f < 4:
                whole = jnp.logical_or(whole, slot == 5 + f)
            block = jnp.where(whole, high, jnp.where(slot == 9 + f, low, block))
        block = jnp.where(diagonal, block, 0.0)
        layer[pl.ds(pl.multiple_of(h * rows, rows), rows), :] = block.astype(jnp.bfloat16)
        return carry

    lax.fori_loop(0, units, place, 0)
    pl.semaphore_wait(ready.at[1], len(near))
    greet(ready.at[2], near)
    for copy in params:
        copy.wait()

    def moments(p, carry):
        for slot in (1, 2):
            landed(slot, p)

        @pl.when(jnp.logical_and(core == FIRST, p == GATE_PIECE))
        def _():
            pl.semaphore_signal(
                gate,
                inc=1,
                device_id={"ep": partner},
                device_id_type=pl.DeviceIdType.MESH,
            )

        def one(i, inner):
            grad_acc, mom_acc = inner
            cols = cols_of(p, i)
            total = pair_sum(0, cols) + decode(1, p, cols, narrow) + decode(2, p, cols, narrow)
            mom_next = MOMENTUM_DECAY * mom[:, cols] + (1.0 - MOMENTUM_DECAY) * total
            gradient[:, cols] = total
            mom[:, cols] = mom_next
            second[:, cols] = (
                SECOND_DECAY * second[:, cols] + (1.0 - SECOND_DECAY) * total * total
            )
            return grad_acc + total * total, mom_acc + mom_next * mom_next

        return lax.fori_loop(0, piece // narrow, one, carry, unroll=True)

    zero = jnp.zeros((rows, narrow), jnp.float32)
    grad_acc, mom_acc = lax.fori_loop(0, pieces, moments, (zero, zero))

    def to_lanes(acc):
        acc = jnp.sum(acc, axis=0, keepdims=True)
        return sum(acc[:, j : j + LANES] for j in range(0, narrow, LANES))

    pl.semaphore_wait(ready.at[2], len(near))
    sums[me, 0:1, :] = to_lanes(grad_acc)
    sums[me, 1:2, :] = to_lanes(mom_acc)
    def hops(offset):
        return min(offset, SIDE - offset)

    offsets = sorted(
        ((up, along) for up in range(SIDE) for along in range(SIDE)),
        key=lambda pair: -hops(pair[0]) - hops(pair[1]),
    )
    for up, along in offsets[:-1]:
        peer = (z + up) % SIDE * SIDE + (x + along) % SIDE
        remote(sums.at[me], sums.at[me], sum_send, sum_recv, "fs", peer).start()
    others = sums.at[pl.ds(0, shards - 1)]
    all_sums = remote(others, others, sum_send, sum_recv, "fs", (me + 1) % shards)
    all_sums.wait_recv()

    entries = rows * columns * shards
    totals = sums[0]
    for s in range(1, shards):
        totals = totals + sums[s]
    mean = jnp.broadcast_to(jnp.sum(totals, axis=1, keepdims=True) / entries, (2, LANES)) + NORM_EPS
    inverse = lax.rsqrt(mean)
    log_mom = 0.5 * jnp.log(mean[1:2, :])
    tail = pl.ds(shape[1] - LANES, LANES)
    biased = slot[:, -LANES:] >= 14
    first = slot[:, -LANES:] == 14
    ends = diagonal[:, -LANES:]

    def settle(h, carry):
        value = in_bias[h] + in_weight[5, h] * log_mom
        high, low = halves(jnp.broadcast_to(value, ends.shape))
        span = pl.ds(pl.multiple_of(h * rows, rows), rows)
        block = jnp.where(ends, jnp.where(first, high, low), 0.0)
        kept = layer[span, tail].astype(jnp.float32)
        layer[span, tail] = jnp.where(biased, block, kept).astype(jnp.bfloat16)
        return carry

    lax.fori_loop(0, units, settle, 0, unroll=True)

    chunks = pass_recv.shape[1]
    width = columns // chunks
    tile = tile_width(width, TILE)
    inv_grad = spread_lanes(inverse[0:1, :], tile)
    inv_mom = spread_lanes(inverse[1:2, :], tile)

    def learned_step(cols):
        grad = gradient[:, cols]
        mom_next = mom[:, cols]
        narrow_old = weight[:, cols]
        inv_root = lax.rsqrt(second[:, cols] + ROOT_EPS)
        highs, lows = [], []
        for value in (
            grad * inv_grad,
            mom_next * inv_mom,
            mom_next * inv_root,
            grad * inv_root,
        ):
            high = value.astype(jnp.bfloat16)
            highs.append(high)
            lows.append((value - high.astype(jnp.float32)).astype(jnp.bfloat16))
        highs.append(narrow_old)
        ones = jnp.ones(grad.shape, jnp.bfloat16)
        features = jnp.concatenate(highs + lows + highs + [ones, ones], axis=0)
        hidden = jnp.dot(layer[...], features, preferred_element_type=jnp.float32)
        directions = [jnp.full(grad.shape, out_bias[0]), jnp.zeros(grad.shape, jnp.float32)]
        magnitudes = [jnp.full(grad.shape, out_bias[1]), jnp.zeros(grad.shape, jnp.float32)]
        for h in range(units):
            active = jnp.maximum(hidden[h * rows : (h + 1) * rows, :], 0.0)
            side = 2 * h // units
            directions[side] = directions[side] + active * out_weight[0, h]
            magnitudes[side] = magnitudes[side] + active * out_weight[1, h]
        direction = directions[0] + directions[1]
        magnitude = magnitudes[0] + magnitudes[1]
        update = STEP_SCALE * direction * jnp.exp(EXP_SCALE * magnitude)
        return (narrow_old.astype(jnp.float32) - update).astype(jnp.bfloat16)

    def rows_of(source):
        return pl.ds(pl.multiple_of(source * rows, rows), rows)

    def block(source, k):
        return gathered.at[rows_of(source), pl.ds(pl.multiple_of(k * width, width), width)]

    def route(k):
        swap = k % 2
        turn = 1 - 2 * (k // 2 % 2)

        def at(first, after):
            up = (z + 2 * SIDE + first * swap + after * (1 - swap)) % SIDE
            along = (x + 2 * SIDE + first * (1 - swap) + after * swap) % SIDE
            return up * SIDE + along

        return at, turn

    def send(source, k, role, recv, peer):
        remote(block(source, k), block(source, k), row_send.at[role], recv, "fs", peer).start()

    def spread(source, k, role, at, way):
        send(source, k, role, pass_recv.at[role, k], at(0, way))
        send(source, k, role, last_recv, at(0, -way))

    def arrive(stage, k, count):
        part = gathered.at[pl.ds(0, count * rows), pl.ds(pl.multiple_of(k * width, width), width)]
        remote(part, part, row_send.at[0], pass_recv.at[stage, k], "fs", me).wait_recv()

    def pass_on(k, role, first):
        at, turn = route(k)
        way = turn if first % 2 == 0 else -turn
        source = at(first * turn, -way)
        send(source, k, role, last_recv, at(0, way))

    def own(k):
        at, turn = route(k)
        send(me, k, 0, pass_recv.at[0, k], at(turn, 0))
        send(me, k, 0, pass_recv.at[0, k], at(-turn, 0))
        spread(me, k, 0, at, turn)

    def relay_one(k):
        at, turn = route(k)
        arrive(0, k, 3)
        source = at(-turn, 0)
        send(source, k, 1, pass_recv.at[1, k], at(turn, 0))
        spread(source, k, 1, at, -turn)
        spread(at(turn, 0), k, 1, at, -turn)
        pass_on(k, 1, 0)

    def relay_two(k):
        at, turn = route(k)
        arrive(1, k, 3)
        spread(at(2, 0), k, 2, at, turn)
        pass_on(k, 2, -1)
        pass_on(k, 2, 1)

    def relay_three(k):
        arrive(2, k, 1)
        pass_on(k, 3, 2)

    def turn_of(t, carry):
        for lag, relay in ((LAG_ONE, relay_one), (LAG_TWO, relay_two), (LAG_THREE, relay_three)):
            k = t - lag

            @pl.when(jnp.logical_and(k >= 0, k < chunks))
            def _(k=k, relay=relay):
                relay(k)

        @pl.when(t < chunks)
        def _():
            def one(i, inner):
                cols = pl.ds(pl.multiple_of(t * width + i * tile, tile), tile)
                gathered[rows_of(me), cols] = learned_step(cols)
                return inner

            lax.fori_loop(0, width // tile, one, 0)
            own(t)

        return carry

    lax.fori_loop(0, chunks + LAG_THREE, turn_of, 0)

    for part in range(2):
        slots = (pl.ds(0, 1), pl.ds(1, ring - 1))[part]
        remote(
            pair_out.at[slots], pair_in.at[slots], pair_send.at[part], pair_recv.at[part, 0], "ep", partner
        ).wait_send()
    for slot in range(3):
        remote(
            ring_out.at[slot], ring_in.at[slot], ring_send.at[slot], ring_recv.at[slot, 0], "ep", partner
        ).wait_send()
        remote(
            scale_out.at[slot], scale_in.at[slot], scale_send.at[slot], ring_recv.at[slot, 0], "ep", partner
        ).wait_send()
    all_sums.wait_send()
    part = gathered.at[pl.ds(0, 8 * rows), :]
    remote(part, part, row_send.at[0], last_recv, "fs", me).wait_recv()
    for role, number in enumerate((4, 6, 4, 1)):
        part = gathered.at[pl.ds(0, number * rows), :]
        remote(
            part, part, row_send.at[role], last_recv, "fs", (me + 1) % shards
        ).wait_send()


def store(gathered, mom, second, gathered_hbm, mom_hbm, second_hbm, sems):
    height = gathered.shape[1] // STORES
    copies = [
        pltpu.make_async_copy(
            gathered.at[:, pl.ds(i * height, height), :],
            gathered_hbm.at[:, pl.ds(i * height, height), :],
            sems.at[i],
        )
        for i in range(STORES)
    ]
    copies.append(pltpu.make_async_copy(mom, mom_hbm, sems.at[STORES]))
    copies.append(pltpu.make_async_copy(second, second_hbm, sems.at[STORES + 1]))
    for copy in copies:
        copy.start()
    for copy in copies:
        copy.wait()


def per_device(groups, grads, counts, weight, mom, second, in_weight, in_bias, out_weight, out_bias):
    rows, columns = mom.shape[1], mom.shape[2]
    ring = groups // CORES
    shards = SIDE * SIDE
    pieces = PIECES
    chunks = CHUNKS
    hbm = pl.BlockSpec(memory_space=pltpu.HBM)
    vmem = pl.BlockSpec(memory_space=pltpu.VMEM)
    results = pl.pallas_call(
        functools.partial(kernel, ring),
        out_shape=(
            pltpu.VMEM((1, rows * shards, columns), jnp.bfloat16),
            pltpu.VMEM(mom.shape, jnp.float32),
            pltpu.VMEM(second.shape, jnp.float32),
        ),
        in_specs=[hbm] * 9,
        out_specs=(vmem, vmem, vmem),
        scratch_shapes=[
            pltpu.SMEM(counts.shape, jnp.int32),
            pltpu.SMEM(in_weight.shape, jnp.float32),
            pltpu.SMEM(in_bias.shape, jnp.float32),
            pltpu.SMEM(out_weight.shape[::-1], jnp.float32),
            pltpu.SMEM(out_bias.shape, jnp.float32),
            pltpu.VMEM((CORES, ring, rows, columns), jnp.bfloat16),
            pltpu.VMEM((rows, columns), jnp.bfloat16),
            pltpu.VMEM((ring, rows, columns), jnp.bfloat16),
            pltpu.VMEM((ring, rows, columns), jnp.bfloat16),
            pltpu.VMEM((ring - 1, rows, columns), jnp.int16),
            pltpu.VMEM((ring - 1, rows, columns), jnp.int16),
            pltpu.VMEM((ring - 1, pieces, 1, LANES), jnp.float32),
            pltpu.VMEM((ring - 1, pieces, 1, LANES), jnp.float32),
            pltpu.VMEM((rows, columns), jnp.float32),
            pltpu.VMEM((shards, 2, LANES), jnp.float32),
            pltpu.VMEM((in_bias.shape[0] * rows, 16 * rows), jnp.bfloat16),
            pltpu.VMEM((rows * columns // pieces * 2 // (4 * LANES) + 1, LANES), jnp.float32),
            pltpu.SemaphoreType.DMA((5,)),
            pltpu.SemaphoreType.DMA((CORES,)),
            pltpu.SemaphoreType.DMA((3,)),
            pltpu.SemaphoreType.DMA((2,)),
            pltpu.SemaphoreType.DMA((2, pieces)),
            pltpu.SemaphoreType.DMA((ring - 1,)),
            pltpu.SemaphoreType.DMA((ring - 1, pieces)),
            pltpu.SemaphoreType.DMA((ring - 1,)),
            pltpu.SemaphoreType.REGULAR,
            pltpu.SemaphoreType.REGULAR((3,)),
            pltpu.SemaphoreType.DMA,
            pltpu.SemaphoreType.DMA,
            pltpu.SemaphoreType.DMA((4,)),
            pltpu.SemaphoreType.DMA((3, chunks)),
            pltpu.SemaphoreType.DMA,
        ],
        compiler_params=pltpu.CompilerParams(
            collective_id=0, has_side_effects=True, vmem_limit_bytes=VMEM_BYTES
        ),
        name="learned_update",
    )(counts, in_weight, in_bias, out_weight.T, out_bias, grads, weight, mom, second)
    return pl.pallas_call(
        store,
        out_shape=[jax.ShapeDtypeStruct(r.shape, r.dtype) for r in results],
        in_specs=[vmem] * 3,
        out_specs=[hbm] * 3,
        scratch_shapes=[pltpu.SemaphoreType.DMA((STORES + 2,))],
        compiler_params=pltpu.CompilerParams(vmem_limit_bytes=1024 * 1024),
        name="store_results",
    )(*results)


def solution(mesh):
    in_specs = (
        P("ep", None, "fs", None),
        P(),
        P("ep", "fs", None),
        P("ep", "fs", None),
        P("ep", "fs", None),
        P(),
        P(),
        P(),
        P(),
    )
    out_specs = (P("ep", None, None), P("ep", "fs", None), P("ep", "fs", None))
    body = functools.partial(per_device, mesh.shape["ep"])
    return jax.shard_map(
        body, mesh=mesh, in_specs=in_specs, out_specs=out_specs, check_vma=False
    )
```
